32 devices in a mesh: gx: 8 (over y, x, core), gy: 4 (over z).
Axes of the slice: x: 2, y: 2, z: 4, core: 2. Of those that a mesh axis runs over, the one named last changes fastest.
Arguments:
- fields: float32 [8, 2048, 2048], P(None, 'gx', 'gy'), may hold values from -6 to 6
- wave_order: int32 [1024], replicated, may hold values from 0 to 1023, as said below
- kept_mask: int32 [1024, 2048], P('gx', 'gy'), may hold values from 0 to 1, as said below
Outputs:
- spectral: float32 [2, 8, 1024, 2048], P(None, None, 'gx', 'gy')
The draws below stay inside these ranges and needn't reach their ends.
Inputs may be any that keep to these rules, and one draw needn't show every extreme that they name: `wave_order`: each x-wavenumber 0 to 1023 once. `kept_mask`: in each row the kept y-wavenumbers q are those with min(q, 2048 - q) up to a bound that does not grow with the row's x-wavenumber.
All inputs are finite; a program needn't handle non-finite values.
Results may differ from the reference program's by a relative error of at most 0.00007.
Values sent between devices are 32-bit elements; how exact they have to be, the bound alone decides.
A program may use at most 192 MiB of HBM per device.

```python
import math
import jax
import jax.numpy as jnp

NX = 2048
NY = 2048
STACK = 8
KX = 1024


def common_draw(key):
    wave_order = jax.random.permutation(jax.random.fold_in(key, 11), KX).astype(jnp.int32)
    radius_x = jax.random.randint(jax.random.fold_in(key, 12), (), KX // 2, KX)
    radius_y = jax.random.randint(jax.random.fold_in(key, 13), (), NY // 4, NY // 2)
    y_waves = jnp.arange(NY, dtype=jnp.int32)
    folded = jnp.minimum(y_waves, NY - y_waves)
    scaled_x = wave_order * 1024 // radius_x
    scaled_y = folded * 1024 // radius_y
    inside = scaled_x[:, None] * scaled_x[:, None] + scaled_y[None, :] * scaled_y[None, :] <= 1024 * 1024
    return (wave_order, inside.astype(jnp.int32))


def draw_wave_order(key, part):
    return common_draw(key)[0]


def draw_kept_mask(key, part):
    return common_draw(key)[1]


def shard_levels(rng, dims, shards, low, top_value):
    gain = 1.0
    for axis_at, parts in shards:
        draws = jax.random.uniform(jax.random.fold_in(jax.random.fold_in(rng, 6), axis_at), (parts,), jnp.float32, low / len(shards), top_value / len(shards))
        gain = gain * jnp.repeat(jnp.exp(draws), dims[axis_at] // parts).reshape((-1,) + (1,) * (len(dims) - 1 - axis_at))
    return gain


def scatter_about(key, extent, scale, reach, split=(), kind=jnp.bfloat16):
    loudness = shard_levels(key, extent, split, -0.22, 0.18) if split else 1.0
    drawn = jax.random.normal(key, extent, jnp.float32) * scale * loudness
    return jnp.minimum(jnp.maximum(drawn, -reach), reach).astype(kind)


def setup_inputs(seed: int = 0) -> dict:
    key_of = jax.random.split(jax.random.key(seed), 4)
    fields = scatter_about(key_of[0], (STACK, NX, NY), 1.0, 6.0, ((1, 8), (2, 4)), jnp.float32)
    wave_order = draw_wave_order(jax.random.fold_in(key_of[3], 71), 0)
    kept_mask = draw_kept_mask(jax.random.fold_in(key_of[3], 71), 0)
    return {"fields": fields, "wave_order": wave_order, "kept_mask": kept_mask}


def reference(fields, wave_order, kept_mask):
    along_x = jnp.fft.fft(fields, axis=1)
    picked = jnp.take(along_x, wave_order, axis=1)
    both = jnp.fft.fft(picked, axis=2) / math.sqrt(NX * NY)
    weight = kept_mask.astype(jnp.float32)
    real_part = jnp.real(both).astype(jnp.float32) * weight
    imag_part = jnp.imag(both).astype(jnp.float32) * weight
    return jnp.stack([real_part, imag_part]).astype(jnp.float32)
```

```python
import functools
import math

import jax
import jax.numpy as jnp
import numpy as np
from jax import lax
from jax.experimental import pallas as pl
from jax.experimental.pallas import tpu as pltpu
from jax.sharding import PartitionSpec as P

NX = 2048
NY = 2048
STACK = 8
KX = 1024


def wave_angles(wave_ids, points, period):
    phases = wave_ids[:, None] * points[None, :] % period
    angles = phases.astype(jnp.float32) * (2.0 * math.pi / period)
    return (jnp.cos(angles), jnp.sin(angles))


def x_terms(cos_table, sin_table, values):
    stack_count, x_count, y_count = values.shape
    waves = cos_table.shape[0]
    table = jnp.concatenate([cos_table, -sin_table], axis=0)
    flat = jnp.transpose(values, (1, 0, 2)).reshape(x_count, stack_count * y_count)
    product = jnp.dot(
        table, flat, precision=lax.Precision.HIGHEST, preferred_element_type=jnp.float32
    )
    product = product.reshape(2, waves, stack_count, y_count)
    return jnp.transpose(product, (1, 0, 2, 3))


def y_terms(cos_table, sin_table, spectra):
    rows, parts, stack_count, y_count = spectra.shape
    waves = cos_table.shape[0]
    table = jnp.concatenate([cos_table, sin_table], axis=0)
    flat = spectra.reshape(rows * parts * stack_count, y_count)
    product = jnp.dot(
        flat, table.T, precision=lax.Precision.HIGHEST, preferred_element_type=jnp.float32
    )
    product = product.reshape(rows, parts, stack_count, 2, waves)
    real_part = product[:, 0, :, 0] + product[:, 1, :, 1]
    imag_part = product[:, 1, :, 0] - product[:, 0, :, 1]
    return jnp.stack([real_part, imag_part], axis=1)


def shards(fields, wave_order, kept_mask):
    x_every = jnp.arange(NX, dtype=jnp.int32)
    x_cos, x_sin = wave_angles(wave_order, x_every, NX)
    partial_terms = x_terms(
        x_cos, x_sin, lax.all_to_all(fields, "gx", split_axis=2, concat_axis=1, tiled=True)
    )
    spectra = lax.all_to_all(partial_terms, "gx", split_axis=0, concat_axis=3, tiled=True)
    y_every = jnp.arange(NY, dtype=jnp.int32)
    y_cos, y_sin = wave_angles(y_every, y_every, NY)
    y_spectra = y_terms(
        y_cos, y_sin, lax.all_to_all(spectra, "gy", split_axis=0, concat_axis=3, tiled=True)
    )
    result = lax.all_to_all(y_spectra, "gy", split_axis=3, concat_axis=0, tiled=True)
    weight = kept_mask.astype(jnp.float32) * (1.0 / math.sqrt(NX * NY))
    arranged = jnp.transpose(result, (1, 2, 0, 3)) * weight[None, None]
    return arranged


LANES = 128
MESH_IDS = pl.DeviceIdType.MESH


def split_halves(values):
    high = values.astype(jnp.bfloat16)
    return high, (values - high.astype(jnp.float32)).astype(jnp.bfloat16)


def table_halves(table):
    high = table.astype(jnp.bfloat16)
    low = (table - high.astype(np.float64)).astype(jnp.bfloat16)
    return jnp.asarray(high), jnp.asarray(low)


def mxu(left, right):
    return jnp.dot(left, right, preferred_element_type=jnp.float32)


def y_tables(y_local, parts):
    points = np.arange(y_local)
    period = y_local * parts
    turns = np.arange(parts)[:, None] * points[None, :] % period * (2.0 * np.pi / period)
    twiddle = jnp.asarray(np.concatenate([np.cos(turns), np.sin(turns)]), jnp.float32)
    angles = points[:, None] * points[None, :] % y_local * (2.0 * np.pi / y_local)
    cos = np.cos(angles).reshape(y_local, parts, -1)
    sin = np.sin(angles).reshape(y_local, parts, -1)
    both = np.concatenate([cos, sin], axis=2).transpose(1, 0, 2)
    high, low = table_halves(both)
    wide = y_local // parts
    order = np.zeros((y_local, y_local), np.float32)
    for residue in range(parts):
        order[residue * wide + np.arange(wide), parts * np.arange(wide) + residue] = 1.0
    return twiddle, high, low, jnp.asarray(order, jnp.bfloat16)


def exchange_kernel(
    gx, gy, levels, chunks,
    fields, order_rows, twiddle, y_high_in, y_low_in, order_in, out,
    order_column, x_high, x_low, lines, split_lines, waves, held, columns, z_high, z_low, spectra,
    y_high, y_low, order, whole_y,
    send_r, recv_r, send_a, recv_a, send_b, recv_b, send_c, recv_c, send_d, recv_d, table_sem,
):
    me = lax.axis_index("gx")
    my = lax.axis_index("gy")
    x_local = fields.shape[1]
    y_local = fields.shape[2]
    rows = out.shape[3]
    first = chunks // 2
    cuts = y_local // LANES
    block = 2 * rows * gy
    nx = gx * x_local
    near = gy // 2
    far_half = (1 - my // near) * near
    near_half = my // near * near
    x_order = (6, 7, 4, 2, 5, 3, 1, 0)
    y_order = (3, 2, 1, 0)

    def partner(index, o):
        total = 0
        for bit in (1, 2, 4):
            total = total + bit * lax.rem(index // bit + o // bit, 2)
        return total

    def move(axis, target, src, dst, send, recv):
        def remote():
            return pltpu.make_async_remote_copy(
                src_ref=src, dst_ref=dst, send_sem=send, recv_sem=recv,
                device_id={axis: target}, device_id_type=MESH_IDS,
            )

        def local():
            return pltpu.make_async_copy(src, dst, recv)

        return remote, local

    def copy_r(c, o):
        to = partner(my, o)
        return move(
            "gy", to, fields.at[first * levels + to], whole_y.at[my],
            send_r.at[c, o], recv_r.at[c, o],
        )

    def copy_a(c, o):
        to = partner(me, o)
        level = c % first * levels + to // cuts
        source = fields if c < first else whole_y
        lane = pl.multiple_of(lax.rem(to, cuts) * LANES, LANES)
        return move(
            "gx", to,
            source.at[level, :, pl.ds(lane, LANES)],
            lines.at[c, pl.ds(pl.multiple_of(me * x_local, x_local), x_local), :],
            send_a.at[c, o], recv_a.at[c, o],
        )

    def copy_b(c, o, late):
        to = partner(me, o)
        lane = pl.multiple_of(lax.rem(me, cuts) * LANES, LANES)
        start = near_half if late else far_half
        half = pl.ds(start, near)
        if c < first:
            landing = held.at[c, half, me // cuts, :, pl.ds(lane, LANES)]
        else:
            piece = c % first * levels + me // cuts
            landing = columns.at[first + start // near, piece, :, :, pl.ds(lane, LANES)]
        return move(
            "gx", to,
            waves.at[c, o, half],
            landing,
            send_b.at[late, c, o], recv_b.at[late, c, o],
        )

    def copy_c(c, o):
        to = partner(my, o)
        return move(
            "gy", to, held.at[c, to], columns.at[c, my], send_c.at[c, o], recv_c.at[c, o]
        )

    def copy_d(c, o):
        to = partner(my, o)
        if c < first:
            landing = out.at[:, pl.ds(c * levels, levels), my]
        else:
            landing = out.at[:, first * levels + my, pl.ds(c % first * levels, levels)]
        return move(
            "gy", to,
            spectra.at[c, o],
            landing,
            send_d.at[c, o], recv_d.at[c, o],
        )

    def start_all(copy, c, offsets):
        for o in offsets:
            remote, local = copy(c, o)
            (remote() if o else local()).start()

    def arrive(copy, c, offsets):
        for o in offsets:
            remote, local = copy(c, o)
            if o:
                remote().wait_recv()
            else:
                local().wait()

    def first_b(c, o):
        return copy_b(c, o, 0)

    def late_b(c, o):
        return copy_b(c, o, 1)

    def circle(phases):
        turns = phases.astype(jnp.float32) * (1.0 / nx)
        halves = jnp.floor(2.0 * turns + 0.5)
        angle = (turns - 0.5 * halves) * (2.0 * math.pi)
        sign = 1.0 - 2.0 * halves * (2.0 - halves)
        square = angle * angle
        cos = jnp.full_like(square, 1.0 / math.factorial(12))
        sin = jnp.full_like(square, 1.0 / math.factorial(13))
        for power in range(10, -1, -2):
            flip = -1.0 if power % 4 else 1.0
            cos = cos * square + flip / math.factorial(power)
            sin = sin * square + flip / math.factorial(power + 1)
        return cos * sign, sin * angle * sign

    def make_table(step, carry):
        waves_at = order_column[pl.ds(pl.multiple_of(step * rows, rows), rows), :]
        points = lax.broadcasted_iota(jnp.int32, (rows, x_local), 1)
        near_waves = jnp.concatenate([waves_at] * (x_local // LANES), axis=1)
        near_cos, near_sin = circle(near_waves * points & (nx - 1))
        blocks = lax.broadcasted_iota(jnp.int32, (rows, LANES), 1) * x_local
        far_cos, far_sin = circle(waves_at * blocks & (nx - 1))
        first = pl.multiple_of(2 * step * rows, rows)
        for j in range(gx):
            cos, sin = far_cos[:, j : j + 1], far_sin[:, j : j + 1]
            lanes = slice(j * x_local, (j + 1) * x_local)
            for part, value in enumerate(
                (cos * near_cos - sin * near_sin, -(sin * near_cos + cos * near_sin))
            ):
                at = pl.ds(pl.multiple_of(first + part * rows, rows), rows)
                high, low = split_halves(value)
                x_high[at, lanes] = high
                x_low[at, lanes] = low
        return carry

    def x_stage(c):
        def split_block(j, carry):
            at = pl.ds(pl.multiple_of(j * x_local, x_local), x_local)
            high, low = split_halves(lines[c, at, :])
            split_lines[at, :LANES] = high
            split_lines[at, LANES:] = low
            return carry

        lax.fori_loop(0, gx, split_block, 0)

        def one(step, carry):
            o = gx - 1 - step
            to = partner(me, o)
            at = pl.ds(pl.multiple_of(to * block, block), block)
            main = mxu(x_high[at, :], split_lines[...])
            rest = mxu(x_low[at, :], split_lines[:, :LANES])
            total = main[:, :LANES] + main[:, LANES:] + rest
            waves[c, o] = total.reshape(gy, 2 * rows, LANES)
            remote, local = first_b(c, o)
            pl.when(o != 0)(lambda: remote().start())
            pl.when(o == 0)(lambda: local().start())
            return carry

        lax.fori_loop(0, gx, one, 0)
        start_all(late_b, c, x_order)

    def y_stage(c):
        size = 16
        span = levels * rows
        for level in range(levels):
            for i in range(0, rows, size):
                re = [columns[c, g, level, i : i + size, :] for g in range(4)]
                im = [columns[c, g, level, rows + i : rows + i + size, :] for g in range(4)]
                re_even, re_odd = re[0] + re[2], re[0] - re[2]
                im_even, im_odd = im[0] + im[2], im[0] - im[2]
                re_sum, re_gap = re[1] + re[3], re[1] - re[3]
                im_sum, im_gap = im[1] + im[3], im[1] - im[3]
                legs = (
                    (re_even + re_sum, im_even + im_sum),
                    (re_odd + im_gap, im_odd - re_gap),
                    (re_even - re_sum, im_even - im_sum),
                    (re_odd - im_gap, im_odd + re_gap),
                )
                for r, (a, b) in enumerate(legs):
                    cos = twiddle[r : r + 1, :]
                    sin = twiddle[gy + r : gy + r + 1, :]
                    for part, value in enumerate((a * cos + b * sin, b * cos - a * sin)):
                        at = part * gy * span + r * span + level * rows + i
                        high, low = split_halves(value)
                        z_high[at : at + size, :] = high
                        z_low[at : at + size, :] = low

        def one(step, carry):
            o = gy - 1 - step
            to = partner(my, o)
            table = y_high[to]
            terms = mxu(z_high[...], table) + mxu(z_low[...], table) + mxu(z_high[...], y_low[to])
            half = gy * span
            wide = y_local // gy
            re = terms[:half, :wide] + terms[half:, wide:]
            im = terms[half:, :wide] - terms[:half, wide:]
            whole = jnp.concatenate(
                [
                    jnp.concatenate([piece[r * span : (r + 1) * span] for r in range(gy)], axis=1)
                    for piece in (re, im)
                ],
                axis=0,
            )
            high, low = split_halves(whole)
            ordered = mxu(high, order[...]) + mxu(low, order[...])
            spectra[c, o] = ordered.reshape(2, levels, rows, y_local)
            remote, local = copy_d(c, o)
            pl.when(o != 0)(lambda: remote().start())
            pl.when(o == 0)(lambda: local().start())
            return carry

        lax.fori_loop(0, gy, one, 0)

    barrier = pltpu.get_barrier_semaphore()
    for axis, index, size in (("gy", my, gy), ("gx", me, gx)):
        for o in range(1, size):
            pl.semaphore_signal(
                barrier, inc=1, device_id={axis: partner(index, o)}, device_id_type=MESH_IDS
            )
    pl.semaphore_wait(barrier, gx + gy - 2)

    start_all(copy_r, 0, y_order)
    start_all(copy_a, 0, x_order)
    tables = [
        pltpu.make_async_copy(src, dst, table_sem.at[i])
        for i, (src, dst) in enumerate(
            ((y_high_in, y_high), (y_low_in, y_low), (order_in, order))
        )
    ]
    for table in tables:
        table.start()
    for i in range(order_rows.shape[0]):
        row = jnp.broadcast_to(order_rows[i : i + 1, :], (LANES, LANES))
        order_column[i * LANES : (i + 1) * LANES, :] = row.T
    lax.fori_loop(0, x_high.shape[0] // (2 * rows), make_table, 0)
    for table in tables:
        table.wait()

    def forward(c):
        arrive(first_b, c, x_order)
        start_all(copy_c, c, (3, 2))
        arrive(late_b, c, x_order)
        start_all(copy_c, c, (1, 0))

    def lines_stage(c):
        arrive(copy_a, c, x_order)
        x_stage(c)

    def columns_stage(c):
        arrive(copy_c, c, y_order)
        y_stage(c)

    lines_stage(0)
    start_all(copy_a, 1, x_order)
    forward(0)
    lines_stage(1)
    arrive(copy_r, 0, y_order)
    start_all(copy_a, 2, x_order)
    start_all(copy_a, 3, x_order)
    forward(1)
    columns_stage(0)
    lines_stage(2)
    lines_stage(3)
    columns_stage(1)
    for c in (2, 3):
        arrive(first_b, c, x_order)
        arrive(late_b, c, x_order)
    y_stage(2)
    y_stage(3)

    def sent(copy, c, offsets):
        for o in offsets:
            if o:
                copy(c, o)[0]().wait_send()

    for c in range(chunks):
        arrive(copy_d, c, y_order)
    sent(copy_r, 0, y_order)
    for c in range(chunks):
        for copy in (copy_a, first_b, late_b):
            sent(copy, c, x_order)
        if c < first:
            sent(copy_c, c, y_order)
        sent(copy_d, c, y_order)


def keep_kernel(scale, spectra, kept_mask, out, kept, sems):
    copies = []
    for piece in range(spectra.shape[0]):
        kept[piece] = spectra[piece] * (kept_mask[...].astype(jnp.float32) * scale)
        copies.append(pltpu.make_async_copy(kept.at[piece], out.at[piece], sems.at[piece]))
        copies[-1].start()
    for copy in copies:
        copy.wait()


def stay(value):
    return pltpu.with_memory_space_constraint(value, pltpu.HBM)


def kernel_shards(gx, gy, fields, wave_order, kept_mask):
    stack, x_local, y_local = fields.shape
    nx, ny = x_local * gx, y_local * gy
    levels = gx * LANES // y_local
    chunks = stack // levels
    rows = wave_order.shape[0] // (gx * gy)
    all_rows = 2 * wave_order.shape[0]
    twiddle, y_high, y_low, order = y_tables(y_local, gy)
    vmem = pl.BlockSpec(memory_space=pltpu.VMEM)
    anywhere = pl.BlockSpec(memory_space=pl.ANY)
    hbm = pl.BlockSpec(memory_space=pl.ANY)
    z_rows = 2 * gy * levels * rows
    spectra = pl.pallas_call(
        functools.partial(exchange_kernel, gx, gy, levels, chunks),
        out_shape=pltpu.VMEM((2, stack, gy, rows, y_local), jnp.float32),
        in_specs=[hbm, vmem, vmem] + [hbm] * 3,
        out_specs=anywhere,
        scratch_shapes=[
            pltpu.VMEM((wave_order.shape[0], LANES), jnp.int32),
            pltpu.VMEM((all_rows, nx), jnp.bfloat16),
            pltpu.VMEM((all_rows, nx), jnp.bfloat16),
            pltpu.VMEM((chunks, nx, LANES), jnp.float32),
            pltpu.VMEM((nx, 2 * LANES), jnp.bfloat16),
            pltpu.VMEM((chunks, gx, gy, 2 * rows, LANES), jnp.float32),
            pltpu.VMEM((chunks, gy, levels, 2 * rows, y_local), jnp.float32),
            pltpu.VMEM((chunks, gy, levels, 2 * rows, y_local), jnp.float32),
            pltpu.VMEM((z_rows, y_local), jnp.bfloat16),
            pltpu.VMEM((z_rows, y_local), jnp.bfloat16),
            pltpu.VMEM((chunks, gy, 2, levels, rows, y_local), jnp.float32),
            pltpu.VMEM(y_high.shape, jnp.bfloat16),
            pltpu.VMEM(y_low.shape, jnp.bfloat16),
            pltpu.VMEM(order.shape, jnp.bfloat16),
            pltpu.VMEM((gy, x_local, y_local), jnp.float32),
        ]
        + [pltpu.SemaphoreType.DMA((1, gy))] * 2
        + [pltpu.SemaphoreType.DMA((chunks, gx))] * 2
        + [pltpu.SemaphoreType.DMA((2, chunks, gx))] * 2
        + [pltpu.SemaphoreType.DMA((chunks, gy))] * 4
        + [pltpu.SemaphoreType.DMA((3,))],
        compiler_params=pltpu.CompilerParams(
            collective_id=0, has_side_effects=True, vmem_limit_bytes=58 * 1024 * 1024
        ),
        name="exchange",
    )(stay(fields), wave_order.reshape(-1, LANES), twiddle, stay(y_high), stay(y_low), stay(order))
    pieces = 2 * stack
    kept = pl.pallas_call(
        functools.partial(keep_kernel, 1.0 / math.sqrt(nx * ny)),
        out_shape=jax.ShapeDtypeStruct((pieces, gy * rows, y_local), jnp.float32),
        in_specs=[vmem, vmem],
        out_specs=anywhere,
        scratch_shapes=[
            pltpu.VMEM((pieces, gy * rows, y_local), jnp.float32),
            pltpu.SemaphoreType.DMA((pieces,)),
        ],
        compiler_params=pltpu.CompilerParams(vmem_limit_bytes=6 * 1024 * 1024),
        name="keep",
    )(spectra.reshape(pieces, gy * rows, y_local), kept_mask)
    return kept.reshape(2, stack, gy * rows, y_local)


def kernel_fits(gx, gy):
    y_local, x_local = NY // gy, NX // gx
    if gx != 8 or gy != 4 or NX & (NX - 1) or y_local % (4 * LANES) or x_local % LANES or gx * LANES % y_local:
        return False
    levels = gx * LANES // y_local
    return STACK == 4 * levels == 2 * gy and KX % (gx * gy * 16) == 0


def solution(mesh):
    gx, gy = mesh.shape["gx"], mesh.shape["gy"]
    body = functools.partial(kernel_shards, gx, gy) if kernel_fits(gx, gy) else shards
    return jax.shard_map(
        body,
        mesh=mesh,
        in_specs=(P(None, "gx", "gy"), P(), P("gx", "gy")),
        out_specs=P(None, None, "gx", "gy"),
        check_vma=False,
    )
```

```python
import functools
import math

import jax
import jax.numpy as jnp
import numpy as np
from jax import lax
from jax.experimental import pallas as pl
from jax.experimental.pallas import tpu as pltpu
from jax.sharding import PartitionSpec as P

NX = 2048
NY = 2048
STACK = 8
KX = 1024


def wave_angles(wave_ids, points, period):
    phases = wave_ids[:, None] * points[None, :] % period
    angles = phases.astype(jnp.float32) * (2.0 * math.pi / period)
    return (jnp.cos(angles), jnp.sin(angles))


def x_terms(cos_table, sin_table, values):
    stack_count, x_count, y_count = values.shape
    waves = cos_table.shape[0]
    table = jnp.concatenate([cos_table, -sin_table], axis=0)
    flat = jnp.transpose(values, (1, 0, 2)).reshape(x_count, stack_count * y_count)
    product = jnp.dot(
        table, flat, precision=lax.Precision.HIGHEST, preferred_element_type=jnp.float32
    )
    product = product.reshape(2, waves, stack_count, y_count)
    return jnp.transpose(product, (1, 0, 2, 3))


def y_terms(cos_table, sin_table, spectra):
    rows, parts, stack_count, y_count = spectra.shape
    waves = cos_table.shape[0]
    table = jnp.concatenate([cos_table, sin_table], axis=0)
    flat = spectra.reshape(rows * parts * stack_count, y_count)
    product = jnp.dot(
        flat, table.T, precision=lax.Precision.HIGHEST, preferred_element_type=jnp.float32
    )
    product = product.reshape(rows, parts, stack_count, 2, waves)
    real_part = product[:, 0, :, 0] + product[:, 1, :, 1]
    imag_part = product[:, 1, :, 0] - product[:, 0, :, 1]
    return jnp.stack([real_part, imag_part], axis=1)


def shards(fields, wave_order, kept_mask):
    x_every = jnp.arange(NX, dtype=jnp.int32)
    x_cos, x_sin = wave_angles(wave_order, x_every, NX)
    partial_terms = x_terms(
        x_cos, x_sin, lax.all_to_all(fields, "gx", split_axis=2, concat_axis=1, tiled=True)
    )
    spectra = lax.all_to_all(partial_terms, "gx", split_axis=0, concat_axis=3, tiled=True)
    y_every = jnp.arange(NY, dtype=jnp.int32)
    y_cos, y_sin = wave_angles(y_every, y_every, NY)
    y_spectra = y_terms(
        y_cos, y_sin, lax.all_to_all(spectra, "gy", split_axis=0, concat_axis=3, tiled=True)
    )
    result = lax.all_to_all(y_spectra, "gy", split_axis=3, concat_axis=0, tiled=True)
    weight = kept_mask.astype(jnp.float32) * (1.0 / math.sqrt(NX * NY))
    arranged = jnp.transpose(result, (1, 2, 0, 3)) * weight[None, None]
    return arranged


LANES = 128
MESH_IDS = pl.DeviceIdType.MESH


def split_halves(values):
    high = values.astype(jnp.bfloat16)
    return high, (values - high.astype(jnp.float32)).astype(jnp.bfloat16)


def table_halves(table):
    high = table.astype(jnp.bfloat16)
    low = (table - high.astype(np.float64)).astype(jnp.bfloat16)
    return jnp.asarray(high), jnp.asarray(low)


def mxu(left, right):
    return jnp.dot(left, right, preferred_element_type=jnp.float32)


def y_tables(y_local, parts):
    points = np.arange(y_local)
    period = y_local * parts
    turns = np.arange(parts)[:, None] * points[None, :] % period * (2.0 * np.pi / period)
    twiddle = jnp.asarray(np.concatenate([np.cos(turns), np.sin(turns)]), jnp.float32)
    angles = points[:, None] * points[None, :] % y_local * (2.0 * np.pi / y_local)
    cos = np.cos(angles).reshape(y_local, parts, -1)
    sin = np.sin(angles).reshape(y_local, parts, -1)
    both = np.concatenate([cos, sin], axis=2).transpose(1, 0, 2)
    high, low = table_halves(both)
    wide = y_local // parts
    order = np.zeros((y_local, y_local), np.float32)
    for residue in range(parts):
        order[residue * wide + np.arange(wide), parts * np.arange(wide) + residue] = 1.0
    return twiddle, high, low, jnp.asarray(order, jnp.bfloat16)


def exchange_kernel(
    gx, gy, levels, chunks,
    fields, order_rows_in, twiddle_in, y_high_in, y_low_in, order_in, out,
    order_rows, twiddle, order_column, x_high, x_low, lines, split_lines, waves, held, columns, z_high, z_low, spectra,
    y_high, y_low, order, whole_y,
    send_r, recv_r, send_a, recv_a, send_b, recv_b, send_c, recv_c, send_d, recv_d, table_sem,
):
    me = lax.axis_index("gx")
    my = lax.axis_index("gy")
    x_local = fields.shape[1]
    y_local = fields.shape[2]
    rows = out.shape[3]
    first = chunks // 2
    cuts = y_local // LANES
    block = 2 * rows * gy
    nx = gx * x_local
    near = gy // 2
    far_half = (1 - my // near) * near
    near_half = my // near * near
    x_order = (6, 7, 4, 2, 5, 3, 1, 0)
    y_order = (3, 2, 1, 0)

    def partner(index, o):
        total = 0
        for bit in (1, 2, 4):
            total = total + bit * lax.rem(index // bit + o // bit, 2)
        return total

    def turn(step):
        inner = lax.rem(my + 1, gy) // 2
        is_first = (3 - step) // 3
        is_second = lax.rem(step, 2) * ((3 - step) // 2)
        is_third = step // 2 * ((4 - step) // 2)
        return is_first * (1 + inner) + is_second * 3 + is_third * (2 - inner)

    def move(axis, target, src, dst, send, recv):
        def remote():
            return pltpu.make_async_remote_copy(
                src_ref=src, dst_ref=dst, send_sem=send, recv_sem=recv,
                device_id={axis: target}, device_id_type=MESH_IDS,
            )

        def local():
            return pltpu.make_async_copy(src, dst, recv)

        return remote, local

    def copy_r(c, o):
        to = partner(my, o)
        return move(
            "gy", to, fields.at[first * levels + to], whole_y.at[my],
            send_r.at[c, o], recv_r.at[c, o],
        )

    def copy_a(c, o):
        to = partner(me, o)
        level = c % first * levels + to // cuts
        source = fields if c < first else whole_y
        lane = pl.multiple_of(lax.rem(to, cuts) * LANES, LANES)
        return move(
            "gx", to,
            source.at[level, :, pl.ds(lane, LANES)],
            lines.at[c, pl.ds(pl.multiple_of(me * x_local, x_local), x_local), :],
            send_a.at[c, o], recv_a.at[c, o],
        )

    def copy_b(c, o, late):
        to = partner(me, o)
        lane = pl.multiple_of(lax.rem(me, cuts) * LANES, LANES)
        start = near_half if late else far_half
        half = pl.ds(start, near)
        if c < first:
            landing = held.at[c, half, me // cuts, :, pl.ds(lane, LANES)]
        else:
            piece = c % first * levels + me // cuts
            landing = columns.at[first + start // near, piece, :, :, pl.ds(lane, LANES)]
        return move(
            "gx", to,
            waves.at[c, o, half],
            landing,
            send_b.at[late, c, o], recv_b.at[late, c, o],
        )

    def copy_c(c, o):
        to = partner(my, o)
        return move(
            "gy", to, held.at[c, to], columns.at[c, my], send_c.at[c, o], recv_c.at[c, o]
        )

    def copy_d(c, o):
        to = partner(my, o)
        if c < first:
            landing = out.at[:, pl.ds(c * levels, levels), my]
        else:
            landing = out.at[:, first * levels + my, pl.ds(c % first * levels, levels)]
        return move(
            "gy", to,
            spectra.at[c, o],
            landing,
            send_d.at[c, o], recv_d.at[c, o],
        )

    def start_all(copy, c, offsets):
        for o in offsets:
            remote, local = copy(c, o)
            (remote() if o else local()).start()

    def arrive(copy, c, offsets):
        for o in offsets:
            remote, local = copy(c, o)
            if o:
                remote().wait_recv()
            else:
                local().wait()

    def first_b(c, o):
        return copy_b(c, o, 0)

    def late_b(c, o):
        return copy_b(c, o, 1)

    def circle(phases):
        turns = phases.astype(jnp.float32) * (1.0 / nx)
        halves = jnp.floor(2.0 * turns + 0.5)
        angle = (turns - 0.5 * halves) * (2.0 * math.pi)
        sign = 1.0 - 2.0 * halves * (2.0 - halves)
        square = angle * angle
        cos = jnp.full_like(square, 1.0 / math.factorial(12))
        sin = jnp.full_like(square, 1.0 / math.factorial(13))
        for power in range(10, -1, -2):
            flip = -1.0 if power % 4 else 1.0
            cos = cos * square + flip / math.factorial(power)
            sin = sin * square + flip / math.factorial(power + 1)
        return cos * sign, sin * angle * sign

    def make_table(step, carry):
        waves_at = order_column[pl.ds(pl.multiple_of(step * rows, rows), rows), :]
        points = lax.broadcasted_iota(jnp.int32, (rows, x_local), 1)
        near_waves = jnp.concatenate([waves_at] * (x_local // LANES), axis=1)
        near_cos, near_sin = circle(near_waves * points & (nx - 1))
        blocks = lax.broadcasted_iota(jnp.int32, (rows, LANES), 1) * x_local
        far_cos, far_sin = circle(waves_at * blocks & (nx - 1))
        first = pl.multiple_of(2 * step * rows, rows)
        for j in range(gx):
            cos, sin = far_cos[:, j : j + 1], far_sin[:, j : j + 1]
            lanes = slice(j * x_local, (j + 1) * x_local)
            for part, value in enumerate(
                (cos * near_cos - sin * near_sin, -(sin * near_cos + cos * near_sin))
            ):
                at = pl.ds(pl.multiple_of(first + part * rows, rows), rows)
                high, low = split_halves(value)
                x_high[at, lanes] = high
                x_low[at, lanes] = low
        return carry

    def x_stage(c):
        def split_block(j, carry):
            at = pl.ds(pl.multiple_of(j * x_local, x_local), x_local)
            high, low = split_halves(lines[c, at, :])
            split_lines[at, :LANES] = high
            split_lines[at, LANES:] = low
            return carry

        lax.fori_loop(0, gx, split_block, 0)

        def one(step, carry):
            o = gx - 1 - step
            to = partner(me, o)
            at = pl.ds(pl.multiple_of(to * block, block), block)
            main = mxu(x_high[at, :], split_lines[...])
            rest = mxu(x_low[at, :], split_lines[:, :LANES])
            total = main[:, :LANES] + main[:, LANES:] + rest
            waves[c, o] = total.reshape(gy, 2 * rows, LANES)
            remote, local = first_b(c, o)
            pl.when(o != 0)(lambda: remote().start())
            pl.when(o == 0)(lambda: local().start())
            return carry

        lax.fori_loop(0, gx, one, 0)
        start_all(late_b, c, x_order)

    def y_stage(c):
        size = 16
        span = levels * rows
        for level in range(levels):
            for i in range(0, rows, size):
                re = [columns[c, g, level, i : i + size, :] for g in range(4)]
                im = [columns[c, g, level, rows + i : rows + i + size, :] for g in range(4)]
                re_even, re_odd = re[0] + re[2], re[0] - re[2]
                im_even, im_odd = im[0] + im[2], im[0] - im[2]
                re_sum, re_gap = re[1] + re[3], re[1] - re[3]
                im_sum, im_gap = im[1] + im[3], im[1] - im[3]
                legs = (
                    (re_even + re_sum, im_even + im_sum),
                    (re_odd + im_gap, im_odd - re_gap),
                    (re_even - re_sum, im_even - im_sum),
                    (re_odd - im_gap, im_odd + re_gap),
                )
                for r, (a, b) in enumerate(legs):
                    cos = twiddle[r : r + 1, :]
                    sin = twiddle[gy + r : gy + r + 1, :]
                    for part, value in enumerate((a * cos + b * sin, b * cos - a * sin)):
                        at = part * gy * span + r * span + level * rows + i
                        high, low = split_halves(value)
                        z_high[at : at + size, :] = high
                        z_low[at : at + size, :] = low

        def one(step, carry):
            o = turn(step)
            to = partner(my, o)
            table = y_high[to]
            terms = mxu(z_high[...], table) + mxu(z_low[...], table) + mxu(z_high[...], y_low[to])
            half = gy * span
            wide = y_local // gy
            re = terms[:half, :wide] + terms[half:, wide:]
            im = terms[half:, :wide] - terms[:half, wide:]
            whole = jnp.concatenate(
                [
                    jnp.concatenate([piece[r * span : (r + 1) * span] for r in range(gy)], axis=1)
                    for piece in (re, im)
                ],
                axis=0,
            )
            high, low = split_halves(whole)
            ordered = mxu(high, order[...]) + mxu(low, order[...])
            spectra[c, o] = ordered.reshape(2, levels, rows, y_local)
            remote, local = copy_d(c, o)
            pl.when(o != 0)(lambda: remote().start())
            pl.when(o == 0)(lambda: local().start())
            return carry

        lax.fori_loop(0, gy, one, 0)

    barrier = pltpu.get_barrier_semaphore()
    for axis, index, size in (("gy", my, gy), ("gx", me, gx)):
        for o in range(1, size):
            pl.semaphore_signal(
                barrier, inc=1, device_id={axis: partner(index, o)}, device_id_type=MESH_IDS
            )
    pl.semaphore_wait(barrier, gx + gy - 2)

    start_all(copy_r, 0, y_order)
    start_all(copy_a, 0, x_order)
    tables = [
        pltpu.make_async_copy(src, dst, table_sem.at[i])
        for i, (src, dst) in enumerate(
            (
                (order_rows_in, order_rows),
                (twiddle_in, twiddle),
                (y_high_in, y_high),
                (y_low_in, y_low),
                (order_in, order),
            )
        )
    ]
    for table in tables:
        table.start()
    tables[0].wait()
    for i in range(order_rows.shape[0]):
        row = jnp.broadcast_to(order_rows[i : i + 1, :], (LANES, LANES))
        order_column[i * LANES : (i + 1) * LANES, :] = row.T
    lax.fori_loop(0, x_high.shape[0] // (2 * rows), make_table, 0)
    for table in tables[1:]:
        table.wait()

    def forward(c):
        arrive(first_b, c, x_order)
        start_all(copy_c, c, (3, 2))
        arrive(late_b, c, x_order)
        start_all(copy_c, c, (1, 0))

    def lines_stage(c):
        arrive(copy_a, c, x_order)
        x_stage(c)

    def columns_stage(c):
        arrive(copy_c, c, y_order)
        y_stage(c)

    lines_stage(0)
    start_all(copy_a, 1, x_order)
    forward(0)
    lines_stage(1)
    arrive(copy_r, 0, y_order)
    start_all(copy_a, 2, x_order)
    start_all(copy_a, 3, x_order)
    forward(1)
    columns_stage(0)
    lines_stage(2)
    lines_stage(3)
    columns_stage(1)
    for c in (2, 3):
        arrive(first_b, c, x_order)
        arrive(late_b, c, x_order)
    y_stage(2)
    y_stage(3)

    def sent(copy, c, offsets):
        for o in offsets:
            if o:
                copy(c, o)[0]().wait_send()

    for c in range(chunks):
        arrive(copy_d, c, y_order)
    sent(copy_r, 0, y_order)
    for c in range(chunks):
        for copy in (copy_a, first_b, late_b):
            sent(copy, c, x_order)
        if c < first:
            sent(copy_c, c, y_order)
        sent(copy_d, c, y_order)


def keep_kernel(scale, spectra, kept_mask, out, kept, sems):
    copies = []
    for piece in range(spectra.shape[0]):
        kept[piece] = spectra[piece] * (kept_mask[...].astype(jnp.float32) * scale)
        copies.append(pltpu.make_async_copy(kept.at[piece], out.at[piece], sems.at[piece]))
        copies[-1].start()
    for copy in copies:
        copy.wait()


def stay(value):
    return pltpu.with_memory_space_constraint(value, pltpu.HBM)


def kernel_shards(gx, gy, fields, wave_order, kept_mask):
    stack, x_local, y_local = fields.shape
    nx, ny = x_local * gx, y_local * gy
    levels = gx * LANES // y_local
    chunks = stack // levels
    rows = wave_order.shape[0] // (gx * gy)
    all_rows = 2 * wave_order.shape[0]
    twiddle, y_high, y_low, order = y_tables(y_local, gy)
    order_rows = wave_order.reshape(-1, LANES)
    vmem = pl.BlockSpec(memory_space=pltpu.VMEM)
    anywhere = pl.BlockSpec(memory_space=pl.ANY)
    hbm = pl.BlockSpec(memory_space=pl.ANY)
    z_rows = 2 * gy * levels * rows
    spectra = pl.pallas_call(
        functools.partial(exchange_kernel, gx, gy, levels, chunks),
        out_shape=pltpu.VMEM((2, stack, gy, rows, y_local), jnp.float32),
        in_specs=[hbm] * 6,
        out_specs=anywhere,
        scratch_shapes=[
            pltpu.VMEM(order_rows.shape, jnp.int32),
            pltpu.VMEM(twiddle.shape, jnp.float32),
            pltpu.VMEM((wave_order.shape[0], LANES), jnp.int32),
            pltpu.VMEM((all_rows, nx), jnp.bfloat16),
            pltpu.VMEM((all_rows, nx), jnp.bfloat16),
            pltpu.VMEM((chunks, nx, LANES), jnp.float32),
            pltpu.VMEM((nx, 2 * LANES), jnp.bfloat16),
            pltpu.VMEM((chunks, gx, gy, 2 * rows, LANES), jnp.float32),
            pltpu.VMEM((chunks, gy, levels, 2 * rows, y_local), jnp.float32),
            pltpu.VMEM((chunks, gy, levels, 2 * rows, y_local), jnp.float32),
            pltpu.VMEM((z_rows, y_local), jnp.bfloat16),
            pltpu.VMEM((z_rows, y_local), jnp.bfloat16),
            pltpu.VMEM((chunks, gy, 2, levels, rows, y_local), jnp.float32),
            pltpu.VMEM(y_high.shape, jnp.bfloat16),
            pltpu.VMEM(y_low.shape, jnp.bfloat16),
            pltpu.VMEM(order.shape, jnp.bfloat16),
            pltpu.VMEM((gy, x_local, y_local), jnp.float32),
        ]
        + [pltpu.SemaphoreType.DMA((1, gy))] * 2
        + [pltpu.SemaphoreType.DMA((chunks, gx))] * 2
        + [pltpu.SemaphoreType.DMA((2, chunks, gx))] * 2
        + [pltpu.SemaphoreType.DMA((chunks, gy))] * 4
        + [pltpu.SemaphoreType.DMA((5,))],
        compiler_params=pltpu.CompilerParams(
            collective_id=0, has_side_effects=True, vmem_limit_bytes=58 * 1024 * 1024
        ),
        name="exchange",
    )(*map(stay, (fields, order_rows, twiddle, y_high, y_low, order)))
    pieces = 2 * stack
    kept = pl.pallas_call(
        functools.partial(keep_kernel, 1.0 / math.sqrt(nx * ny)),
        out_shape=jax.ShapeDtypeStruct((pieces, gy * rows, y_local), jnp.float32),
        in_specs=[vmem, vmem],
        out_specs=anywhere,
        scratch_shapes=[
            pltpu.VMEM((pieces, gy * rows, y_local), jnp.float32),
            pltpu.SemaphoreType.DMA((pieces,)),
        ],
        compiler_params=pltpu.CompilerParams(vmem_limit_bytes=6 * 1024 * 1024),
        name="keep",
    )(spectra.reshape(pieces, gy * rows, y_local), kept_mask)
    return kept.reshape(2, stack, gy * rows, y_local)


def kernel_fits(gx, gy):
    y_local, x_local = NY // gy, NX // gx
    if gx != 8 or gy != 4 or NX & (NX - 1) or y_local % (4 * LANES) or x_local % LANES or gx * LANES % y_local:
        return False
    levels = gx * LANES // y_local
    return STACK == 4 * levels == 2 * gy and KX % (gx * gy * 16) == 0


def solution(mesh):
    gx, gy = mesh.shape["gx"], mesh.shape["gy"]
    body = functools.partial(kernel_shards, gx, gy) if kernel_fits(gx, gy) else shards
    return jax.shard_map(
        body,
        mesh=mesh,
        in_specs=(P(None, "gx", "gy"), P(), P("gx", "gy")),
        out_specs=P(None, None, "gx", "gy"),
        check_vma=False,
    )
```

```python
import functools
import math

import jax
import jax.numpy as jnp
import numpy as np
from jax import lax
from jax.experimental import pallas as pl
from jax.experimental.pallas import tpu as pltpu
from jax.sharding import PartitionSpec as P

NX = 2048
NY = 2048
STACK = 8
KX = 1024


def wave_angles(wave_ids, points, period):
    phases = wave_ids[:, None] * points[None, :] % period
    angles = phases.astype(jnp.float32) * (2.0 * math.pi / period)
    return (jnp.cos(angles), jnp.sin(angles))


def x_terms(cos_table, sin_table, values):
    stack_count, x_count, y_count = values.shape
    waves = cos_table.shape[0]
    table = jnp.concatenate([cos_table, -sin_table], axis=0)
    flat = jnp.transpose(values, (1, 0, 2)).reshape(x_count, stack_count * y_count)
    product = jnp.dot(
        table, flat, precision=lax.Precision.HIGHEST, preferred_element_type=jnp.float32
    )
    product = product.reshape(2, waves, stack_count, y_count)
    return jnp.transpose(product, (1, 0, 2, 3))


def y_terms(cos_table, sin_table, spectra):
    rows, parts, stack_count, y_count = spectra.shape
    waves = cos_table.shape[0]
    table = jnp.concatenate([cos_table, sin_table], axis=0)
    flat = spectra.reshape(rows * parts * stack_count, y_count)
    product = jnp.dot(
        flat, table.T, precision=lax.Precision.HIGHEST, preferred_element_type=jnp.float32
    )
    product = product.reshape(rows, parts, stack_count, 2, waves)
    real_part = product[:, 0, :, 0] + product[:, 1, :, 1]
    imag_part = product[:, 1, :, 0] - product[:, 0, :, 1]
    return jnp.stack([real_part, imag_part], axis=1)


def shards(fields, wave_order, kept_mask):
    x_every = jnp.arange(NX, dtype=jnp.int32)
    x_cos, x_sin = wave_angles(wave_order, x_every, NX)
    partial_terms = x_terms(
        x_cos, x_sin, lax.all_to_all(fields, "gx", split_axis=2, concat_axis=1, tiled=True)
    )
    spectra = lax.all_to_all(partial_terms, "gx", split_axis=0, concat_axis=3, tiled=True)
    y_every = jnp.arange(NY, dtype=jnp.int32)
    y_cos, y_sin = wave_angles(y_every, y_every, NY)
    y_spectra = y_terms(
        y_cos, y_sin, lax.all_to_all(spectra, "gy", split_axis=0, concat_axis=3, tiled=True)
    )
    result = lax.all_to_all(y_spectra, "gy", split_axis=3, concat_axis=0, tiled=True)
    weight = kept_mask.astype(jnp.float32) * (1.0 / math.sqrt(NX * NY))
    arranged = jnp.transpose(result, (1, 2, 0, 3)) * weight[None, None]
    return arranged


LANES = 128
MESH_IDS = pl.DeviceIdType.MESH


def split_halves(values):
    high = values.astype(jnp.bfloat16)
    return high, (values - high.astype(jnp.float32)).astype(jnp.bfloat16)


def table_halves(table):
    high = table.astype(jnp.bfloat16)
    low = (table - high.astype(np.float64)).astype(jnp.bfloat16)
    return jnp.asarray(high), jnp.asarray(low)


def mxu(left, right):
    return jnp.dot(left, right, preferred_element_type=jnp.float32)


def y_tables(y_local, parts):
    points = np.arange(y_local)
    period = y_local * parts
    turns = np.arange(parts)[:, None] * points[None, :] % period * (2.0 * np.pi / period)
    twiddle = jnp.asarray(np.concatenate([np.cos(turns), np.sin(turns)]), jnp.float32)
    angles = points[:, None] * points[None, :] % y_local * (2.0 * np.pi / y_local)
    cos = np.cos(angles).reshape(y_local, parts, -1)
    sin = np.sin(angles).reshape(y_local, parts, -1)
    both = np.concatenate([cos, sin], axis=2).transpose(1, 0, 2)
    high, low = table_halves(both)
    wide = y_local // parts
    order = np.zeros((y_local, y_local), np.float32)
    for residue in range(parts):
        order[residue * wide + np.arange(wide), parts * np.arange(wide) + residue] = 1.0
    return twiddle, high, low, jnp.asarray(order, jnp.bfloat16)


def exchange_kernel(
    gx, gy, levels, chunks,
    fields, order_rows_in, twiddle_in, y_high_in, y_low_in, order_in, out,
    order_rows, twiddle, order_column, x_high, x_low, lines, split_lines, waves, held, columns, z_high, z_low, spectra,
    y_high, y_low, order, whole_y,
    send_r, recv_r, send_a, recv_a, send_b, recv_b, send_c, recv_c, send_d, recv_d, table_sem, go,
):
    me = lax.axis_index("gx")
    my = lax.axis_index("gy")
    x_local = fields.shape[1]
    y_local = fields.shape[2]
    rows = out.shape[3]
    first = chunks // 2
    cuts = y_local // LANES
    block = 2 * rows * gy
    nx = gx * x_local
    near = gy // 2
    far_half = (1 - my // near) * near
    near_half = my // near * near
    x_order = (6, 7, 4, 2, 5, 3, 1, 0)
    y_order = (3, 2, 1, 0)

    def partner(index, o):
        total = 0
        for bit in (1, 2, 4):
            total = total + bit * lax.rem(index // bit + o // bit, 2)
        return total

    def inner_at(y_index):
        return lax.rem(y_index + 1, gy) // 2

    def lone_at(x_index, y_index):
        return inner_at(y_index) * (1 - lax.rem(x_index + y_index, 2))

    def turn(step):
        inner = inner_at(my)
        is_first = (3 - step) // 3
        is_second = lax.rem(step, 2) * ((3 - step) // 2)
        is_third = step // 2 * ((4 - step) // 2)
        return is_first * (1 + inner) + is_second * 3 + is_third * (2 - inner)

    def move(axis, target, src, dst, send, recv):
        def remote():
            return pltpu.make_async_remote_copy(
                src_ref=src, dst_ref=dst, send_sem=send, recv_sem=recv,
                device_id={axis: target}, device_id_type=MESH_IDS,
            )

        def local():
            return pltpu.make_async_copy(src, dst, recv)

        return remote, local

    def copy_r(c, o):
        to = partner(my, o)
        return move(
            "gy", to, fields.at[first * levels + to], whole_y.at[my],
            send_r.at[c, o], recv_r.at[c, o],
        )

    def copy_a(c, o):
        to = partner(me, o)
        level = c % first * levels + to // cuts
        source = fields if c < first else whole_y
        lane = pl.multiple_of(lax.rem(to, cuts) * LANES, LANES)
        return move(
            "gx", to,
            source.at[level, :, pl.ds(lane, LANES)],
            lines.at[c, pl.ds(pl.multiple_of(me * x_local, x_local), x_local), :],
            send_a.at[c, o], recv_a.at[c, o],
        )

    def copy_b(c, o, late):
        to = partner(me, o)
        lane = pl.multiple_of(lax.rem(me, cuts) * LANES, LANES)
        start = near_half if late else far_half
        half = pl.ds(start, near)
        if c < first:
            landing = held.at[c, half, me // cuts, :, pl.ds(lane, LANES)]
        else:
            piece = c % first * levels + me // cuts
            landing = columns.at[first + start // near, piece, :, :, pl.ds(lane, LANES)]
        return move(
            "gx", to,
            waves.at[c, o, half],
            landing,
            send_b.at[late, c, o], recv_b.at[late, c, o],
        )

    def copy_c(c, o):
        to = partner(my, o)
        return move(
            "gy", to, held.at[c, to], columns.at[c, my], send_c.at[c, o], recv_c.at[c, o]
        )

    def copy_d(c, o):
        to = partner(my, o)
        if c < first:
            landing = out.at[:, pl.ds(c * levels, levels), my]
        else:
            landing = out.at[:, first * levels + my, pl.ds(c % first * levels, levels)]
        return move(
            "gy", to,
            spectra.at[c, o],
            landing,
            send_d.at[c, o], recv_d.at[c, o],
        )

    def start_all(copy, c, offsets):
        for o in offsets:
            remote, local = copy(c, o)
            (remote() if o else local()).start()

    def arrive(copy, c, offsets):
        for o in offsets:
            remote, local = copy(c, o)
            if o:
                remote().wait_recv()
            else:
                local().wait()

    def first_b(c, o):
        return copy_b(c, o, 0)

    def late_b(c, o):
        return copy_b(c, o, 1)

    def circle(phases):
        turns = phases.astype(jnp.float32) * (1.0 / nx)
        halves = jnp.floor(2.0 * turns + 0.5)
        angle = (turns - 0.5 * halves) * (2.0 * math.pi)
        sign = 1.0 - 2.0 * halves * (2.0 - halves)
        square = angle * angle
        cos = jnp.full_like(square, 1.0 / math.factorial(12))
        sin = jnp.full_like(square, 1.0 / math.factorial(13))
        for power in range(10, -1, -2):
            flip = -1.0 if power % 4 else 1.0
            cos = cos * square + flip / math.factorial(power)
            sin = sin * square + flip / math.factorial(power + 1)
        return cos * sign, sin * angle * sign

    def make_table(step, carry):
        waves_at = order_column[pl.ds(pl.multiple_of(step * rows, rows), rows), :]
        points = lax.broadcasted_iota(jnp.int32, (rows, x_local), 1)
        near_waves = jnp.concatenate([waves_at] * (x_local // LANES), axis=1)
        near_cos, near_sin = circle(near_waves * points & (nx - 1))
        blocks = lax.broadcasted_iota(jnp.int32, (rows, LANES), 1) * x_local
        far_cos, far_sin = circle(waves_at * blocks & (nx - 1))
        first = pl.multiple_of(2 * step * rows, rows)
        for j in range(gx):
            cos, sin = far_cos[:, j : j + 1], far_sin[:, j : j + 1]
            lanes = slice(j * x_local, (j + 1) * x_local)
            for part, value in enumerate(
                (cos * near_cos - sin * near_sin, -(sin * near_cos + cos * near_sin))
            ):
                at = pl.ds(pl.multiple_of(first + part * rows, rows), rows)
                high, low = split_halves(value)
                x_high[at, lanes] = high
                x_low[at, lanes] = low
        return carry

    def x_stage(c):
        def split_block(j, carry):
            at = pl.ds(pl.multiple_of(j * x_local, x_local), x_local)
            high, low = split_halves(lines[c, at, :])
            split_lines[at, :LANES] = high
            split_lines[at, LANES:] = low
            return carry

        lax.fori_loop(0, gx, split_block, 0)

        def one(step, carry):
            o = gx - 1 - step
            to = partner(me, o)
            at = pl.ds(pl.multiple_of(to * block, block), block)
            main = mxu(x_high[at, :], split_lines[...])
            rest = mxu(x_low[at, :], split_lines[:, :LANES])
            total = main[:, :LANES] + main[:, LANES:] + rest
            waves[c, o] = total.reshape(gy, 2 * rows, LANES)
            remote, local = first_b(c, o)
            pl.when(o != 0)(lambda: remote().start())
            pl.when(o == 0)(lambda: local().start())
            return carry

        lax.fori_loop(0, gx, one, 0)
        start_all(late_b, c, x_order)

    def y_stage(c):
        size = 16
        span = levels * rows
        for level in range(levels):
            for i in range(0, rows, size):
                re = [columns[c, g, level, i : i + size, :] for g in range(4)]
                im = [columns[c, g, level, rows + i : rows + i + size, :] for g in range(4)]
                re_even, re_odd = re[0] + re[2], re[0] - re[2]
                im_even, im_odd = im[0] + im[2], im[0] - im[2]
                re_sum, re_gap = re[1] + re[3], re[1] - re[3]
                im_sum, im_gap = im[1] + im[3], im[1] - im[3]
                legs = (
                    (re_even + re_sum, im_even + im_sum),
                    (re_odd + im_gap, im_odd - re_gap),
                    (re_even - re_sum, im_even - im_sum),
                    (re_odd - im_gap, im_odd + re_gap),
                )
                for r, (a, b) in enumerate(legs):
                    cos = twiddle[r : r + 1, :]
                    sin = twiddle[gy + r : gy + r + 1, :]
                    for part, value in enumerate((a * cos + b * sin, b * cos - a * sin)):
                        at = part * gy * span + r * span + level * rows + i
                        high, low = split_halves(value)
                        z_high[at : at + size, :] = high
                        z_low[at : at + size, :] = low

        def one(step, carry):
            o = turn(step)
            to = partner(my, o)
            table = y_high[to]
            terms = mxu(z_high[...], table) + mxu(z_low[...], table) + mxu(z_high[...], y_low[to])
            half = gy * span
            wide = y_local // gy
            re = terms[:half, :wide] + terms[half:, wide:]
            im = terms[half:, :wide] - terms[:half, wide:]
            whole = jnp.concatenate(
                [
                    jnp.concatenate([piece[r * span : (r + 1) * span] for r in range(gy)], axis=1)
                    for piece in (re, im)
                ],
                axis=0,
            )
            high, low = split_halves(whole)
            ordered = mxu(high, order[...]) + mxu(low, order[...])
            spectra[c, o] = ordered.reshape(2, levels, rows, y_local)
            remote, local = copy_d(c, o)
            pl.when(o != 0)(lambda: remote().start())
            pl.when(o == 0)(lambda: local().start())
            return carry

        lax.fori_loop(0, gy, one, 0)

    barrier = pltpu.get_barrier_semaphore()
    lone = lone_at(me, my)

    def greet(semaphore, axis, target):
        pl.semaphore_signal(
            semaphore, inc=1, device_id={axis: target}, device_id_type=MESH_IDS
        )

    greet(barrier, "gy", partner(my, gy - 1))
    for o in range(1, gy - 1):
        to = partner(my, o)
        pl.when(lone_at(me, to) == 0)(functools.partial(greet, barrier, "gy", to))
    for o in range(1, gx):
        to = partner(me, o)
        pl.when(lone_at(to, my) == 0)(functools.partial(greet, barrier, "gx", to))
    pl.semaphore_wait(barrier, 1 + (1 - lone) * (gx + gy - 3))
    start_all(copy_r, 0, (gy - 1,))

    def release():
        for o in range(1, gy - 1):
            to = partner(my, o)
            pl.when(lone_at(me, to) * (1 - inner_at(my)) == 1)(
                functools.partial(greet, go, "gy", to)
            )
        for o in range(1, gx):
            to = partner(me, o)
            pl.when(lone_at(to, my) == 1)(functools.partial(greet, go, "gx", to))
        to = partner(my, gy - 1)
        pl.when(lone_at(me, to) * (1 - inner_at(my)) == 1)(
            functools.partial(greet, go, "gy", to)
        )

    pl.when(lone == 0)(release)
    pl.when(lone == 1)(lambda: pl.semaphore_wait(go, gx // 2 + gy // 2))
    start_all(copy_r, 0, y_order[1:])
    start_all(copy_a, 0, x_order)
    tables = [
        pltpu.make_async_copy(src, dst, table_sem.at[i])
        for i, (src, dst) in enumerate(
            (
                (order_rows_in, order_rows),
                (twiddle_in, twiddle),
                (y_high_in, y_high),
                (y_low_in, y_low),
                (order_in, order),
            )
        )
    ]
    for table in tables:
        table.start()
    tables[0].wait()
    for i in range(order_rows.shape[0]):
        row = jnp.broadcast_to(order_rows[i : i + 1, :], (LANES, LANES))
        order_column[i * LANES : (i + 1) * LANES, :] = row.T
    lax.fori_loop(0, x_high.shape[0] // (2 * rows), make_table, 0)
    for table in tables[1:]:
        table.wait()

    def forward(c):
        arrive(first_b, c, x_order)
        start_all(copy_c, c, (3, 2))
        arrive(late_b, c, x_order)
        start_all(copy_c, c, (1, 0))

    def lines_stage(c):
        arrive(copy_a, c, x_order)
        x_stage(c)

    def columns_stage(c):
        arrive(copy_c, c, y_order)
        y_stage(c)

    lines_stage(0)
    start_all(copy_a, 1, x_order)
    forward(0)
    lines_stage(1)
    arrive(copy_r, 0, y_order)
    start_all(copy_a, 2, x_order)
    start_all(copy_a, 3, x_order)
    forward(1)
    columns_stage(0)
    lines_stage(2)
    lines_stage(3)
    columns_stage(1)
    for c in (2, 3):
        arrive(first_b, c, x_order)
        arrive(late_b, c, x_order)
    y_stage(2)
    y_stage(3)

    def sent(copy, c, offsets):
        for o in offsets:
            if o:
                copy(c, o)[0]().wait_send()

    for c in range(chunks):
        arrive(copy_d, c, y_order)
    sent(copy_r, 0, y_order)
    for c in range(chunks):
        for copy in (copy_a, first_b, late_b):
            sent(copy, c, x_order)
        if c < first:
            sent(copy_c, c, y_order)
        sent(copy_d, c, y_order)


def keep_kernel(scale, spectra, kept_mask, out, kept, sems):
    copies = []
    for piece in range(spectra.shape[0]):
        kept[piece] = spectra[piece] * (kept_mask[...].astype(jnp.float32) * scale)
        copies.append(pltpu.make_async_copy(kept.at[piece], out.at[piece], sems.at[piece]))
        copies[-1].start()
    for copy in copies:
        copy.wait()


def stay(value):
    return pltpu.with_memory_space_constraint(value, pltpu.HBM)


def kernel_shards(gx, gy, fields, wave_order, kept_mask):
    stack, x_local, y_local = fields.shape
    nx, ny = x_local * gx, y_local * gy
    levels = gx * LANES // y_local
    chunks = stack // levels
    rows = wave_order.shape[0] // (gx * gy)
    all_rows = 2 * wave_order.shape[0]
    twiddle, y_high, y_low, order = y_tables(y_local, gy)
    order_rows = wave_order.reshape(-1, LANES)
    vmem = pl.BlockSpec(memory_space=pltpu.VMEM)
    anywhere = pl.BlockSpec(memory_space=pl.ANY)
    hbm = pl.BlockSpec(memory_space=pl.ANY)
    z_rows = 2 * gy * levels * rows
    spectra = pl.pallas_call(
        functools.partial(exchange_kernel, gx, gy, levels, chunks),
        out_shape=pltpu.VMEM((2, stack, gy, rows, y_local), jnp.float32),
        in_specs=[hbm] * 6,
        out_specs=anywhere,
        scratch_shapes=[
            pltpu.VMEM(order_rows.shape, jnp.int32),
            pltpu.VMEM(twiddle.shape, jnp.float32),
            pltpu.VMEM((wave_order.shape[0], LANES), jnp.int32),
            pltpu.VMEM((all_rows, nx), jnp.bfloat16),
            pltpu.VMEM((all_rows, nx), jnp.bfloat16),
            pltpu.VMEM((chunks, nx, LANES), jnp.float32),
            pltpu.VMEM((nx, 2 * LANES), jnp.bfloat16),
            pltpu.VMEM((chunks, gx, gy, 2 * rows, LANES), jnp.float32),
            pltpu.VMEM((chunks, gy, levels, 2 * rows, y_local), jnp.float32),
            pltpu.VMEM((chunks, gy, levels, 2 * rows, y_local), jnp.float32),
            pltpu.VMEM((z_rows, y_local), jnp.bfloat16),
            pltpu.VMEM((z_rows, y_local), jnp.bfloat16),
            pltpu.VMEM((chunks, gy, 2, levels, rows, y_local), jnp.float32),
            pltpu.VMEM(y_high.shape, jnp.bfloat16),
            pltpu.VMEM(y_low.shape, jnp.bfloat16),
            pltpu.VMEM(order.shape, jnp.bfloat16),
            pltpu.VMEM((gy, x_local, y_local), jnp.float32),
        ]
        + [pltpu.SemaphoreType.DMA((1, gy))] * 2
        + [pltpu.SemaphoreType.DMA((chunks, gx))] * 2
        + [pltpu.SemaphoreType.DMA((2, chunks, gx))] * 2
        + [pltpu.SemaphoreType.DMA((chunks, gy))] * 4
        + [pltpu.SemaphoreType.DMA((5,)), pltpu.SemaphoreType.REGULAR],
        compiler_params=pltpu.CompilerParams(
            collective_id=0, has_side_effects=True, vmem_limit_bytes=58 * 1024 * 1024
        ),
        name="exchange",
    )(*map(stay, (fields, order_rows, twiddle, y_high, y_low, order)))
    pieces = 2 * stack
    kept = pl.pallas_call(
        functools.partial(keep_kernel, 1.0 / math.sqrt(nx * ny)),
        out_shape=jax.ShapeDtypeStruct((pieces, gy * rows, y_local), jnp.float32),
        in_specs=[vmem, vmem],
        out_specs=anywhere,
        scratch_shapes=[
            pltpu.VMEM((pieces, gy * rows, y_local), jnp.float32),
            pltpu.SemaphoreType.DMA((pieces,)),
        ],
        compiler_params=pltpu.CompilerParams(vmem_limit_bytes=6 * 1024 * 1024),
        name="keep",
    )(spectra.reshape(pieces, gy * rows, y_local), kept_mask)
    return kept.reshape(2, stack, gy * rows, y_local)


def kernel_fits(gx, gy):
    y_local, x_local = NY // gy, NX // gx
    if gx != 8 or gy != 4 or NX & (NX - 1) or y_local % (4 * LANES) or x_local % LANES or gx * LANES % y_local:
        return False
    levels = gx * LANES // y_local
    return STACK == 4 * levels == 2 * gy and KX % (gx * gy * 16) == 0


def solution(mesh):
    gx, gy = mesh.shape["gx"], mesh.shape["gy"]
    body = functools.partial(kernel_shards, gx, gy) if kernel_fits(gx, gy) else shards
    return jax.shard_map(
        body,
        mesh=mesh,
        in_specs=(P(None, "gx", "gy"), P(), P("gx", "gy")),
        out_specs=P(None, None, "gx", "gy"),
        check_vma=False,
    )
```

```python
import functools
import math

import jax
import jax.numpy as jnp
import numpy as np
from jax import lax
from jax.experimental import pallas as pl
from jax.experimental.pallas import tpu as pltpu
from jax.sharding import PartitionSpec as P

NX = 2048
NY = 2048
STACK = 8
KX = 1024


def wave_angles(wave_ids, points, period):
    phases = wave_ids[:, None] * points[None, :] % period
    angles = phases.astype(jnp.float32) * (2.0 * math.pi / period)
    return (jnp.cos(angles), jnp.sin(angles))


def x_terms(cos_table, sin_table, values):
    stack_count, x_count, y_count = values.shape
    waves = cos_table.shape[0]
    table = jnp.concatenate([cos_table, -sin_table], axis=0)
    flat = jnp.transpose(values, (1, 0, 2)).reshape(x_count, stack_count * y_count)
    product = jnp.dot(
        table, flat, precision=lax.Precision.HIGHEST, preferred_element_type=jnp.float32
    )
    product = product.reshape(2, waves, stack_count, y_count)
    return jnp.transpose(product, (1, 0, 2, 3))


def y_terms(cos_table, sin_table, spectra):
    rows, parts, stack_count, y_count = spectra.shape
    waves = cos_table.shape[0]
    table = jnp.concatenate([cos_table, sin_table], axis=0)
    flat = spectra.reshape(rows * parts * stack_count, y_count)
    product = jnp.dot(
        flat, table.T, precision=lax.Precision.HIGHEST, preferred_element_type=jnp.float32
    )
    product = product.reshape(rows, parts, stack_count, 2, waves)
    real_part = product[:, 0, :, 0] + product[:, 1, :, 1]
    imag_part = product[:, 1, :, 0] - product[:, 0, :, 1]
    return jnp.stack([real_part, imag_part], axis=1)


def shards(fields, wave_order, kept_mask):
    x_every = jnp.arange(NX, dtype=jnp.int32)
    x_cos, x_sin = wave_angles(wave_order, x_every, NX)
    partial_terms = x_terms(
        x_cos, x_sin, lax.all_to_all(fields, "gx", split_axis=2, concat_axis=1, tiled=True)
    )
    spectra = lax.all_to_all(partial_terms, "gx", split_axis=0, concat_axis=3, tiled=True)
    y_every = jnp.arange(NY, dtype=jnp.int32)
    y_cos, y_sin = wave_angles(y_every, y_every, NY)
    y_spectra = y_terms(
        y_cos, y_sin, lax.all_to_all(spectra, "gy", split_axis=0, concat_axis=3, tiled=True)
    )
    result = lax.all_to_all(y_spectra, "gy", split_axis=3, concat_axis=0, tiled=True)
    weight = kept_mask.astype(jnp.float32) * (1.0 / math.sqrt(NX * NY))
    arranged = jnp.transpose(result, (1, 2, 0, 3)) * weight[None, None]
    return arranged


LANES = 128
MESH_IDS = pl.DeviceIdType.MESH


def split_halves(values):
    high = values.astype(jnp.bfloat16)
    return high, (values - high.astype(jnp.float32)).astype(jnp.bfloat16)


def table_halves(table):
    high = table.astype(jnp.bfloat16)
    low = (table - high.astype(np.float64)).astype(jnp.bfloat16)
    return jnp.asarray(high), jnp.asarray(low)


def mxu(left, right):
    return jnp.dot(left, right, preferred_element_type=jnp.float32)


def y_tables(y_local, parts):
    points = np.arange(y_local)
    period = y_local * parts
    turns = np.arange(parts)[:, None] * points[None, :] % period * (2.0 * np.pi / period)
    twiddle = jnp.asarray(np.concatenate([np.cos(turns), np.sin(turns)]), jnp.float32)
    angles = points[:, None] * points[None, :] % y_local * (2.0 * np.pi / y_local)
    cos = np.cos(angles).reshape(y_local, parts, -1)
    sin = np.sin(angles).reshape(y_local, parts, -1)
    both = np.concatenate([cos, sin], axis=2).transpose(1, 0, 2)
    high, low = table_halves(both)
    wide = y_local // parts
    order = np.zeros((y_local, y_local), np.float32)
    for residue in range(parts):
        order[residue * wide + np.arange(wide), parts * np.arange(wide) + residue] = 1.0
    return twiddle, high, low, jnp.asarray(order, jnp.bfloat16)


def exchange_kernel(
    gx, gy, levels, chunks,
    fields, order_rows_in, twiddle_in, y_high_in, y_low_in, order_in, out,
    order_rows, twiddle, order_column, x_high, x_low, lines, split_lines, waves, held, columns, z_high, z_low, spectra,
    y_high, y_low, order, whole_y,
    send_r, recv_r, send_a, recv_a, send_b, recv_b, send_c, recv_c, send_d, recv_d, table_sem, go,
):
    me = lax.axis_index("gx")
    my = lax.axis_index("gy")
    x_local = fields.shape[1]
    y_local = fields.shape[2]
    rows = out.shape[3]
    first = chunks // 2
    cuts = y_local // LANES
    block = 2 * rows * gy
    nx = gx * x_local
    near = gy // 2
    far_half = (1 - my // near) * near
    near_half = my // near * near
    x_order = (6, 7, 4, 2, 5, 3, 1, 0)
    y_order = (3, 2, 1, 0)

    def partner(index, o):
        total = 0
        for bit in (1, 2, 4):
            total = total + bit * lax.rem(index // bit + o // bit, 2)
        return total

    def inner_at(y_index):
        return lax.rem(y_index + 1, gy) // 2

    def lone_at(x_index, y_index):
        return inner_at(y_index) * lax.rem(x_index, 2)

    def turn(step):
        inner = inner_at(my)
        is_first = (3 - step) // 3
        is_second = lax.rem(step, 2) * ((3 - step) // 2)
        is_third = step // 2 * ((4 - step) // 2)
        return is_first * (1 + inner) + is_second * 3 + is_third * (2 - inner)

    def move(axis, target, src, dst, send, recv):
        def remote():
            return pltpu.make_async_remote_copy(
                src_ref=src, dst_ref=dst, send_sem=send, recv_sem=recv,
                device_id={axis: target}, device_id_type=MESH_IDS,
            )

        def local():
            return pltpu.make_async_copy(src, dst, recv)

        return remote, local

    def copy_r(c, o):
        to = partner(my, o)
        return move(
            "gy", to, fields.at[first * levels + to], whole_y.at[my],
            send_r.at[c, o], recv_r.at[c, o],
        )

    def copy_a(c, o):
        to = partner(me, o)
        level = c % first * levels + to // cuts
        source = fields if c < first else whole_y
        lane = pl.multiple_of(lax.rem(to, cuts) * LANES, LANES)
        return move(
            "gx", to,
            source.at[level, :, pl.ds(lane, LANES)],
            lines.at[c, pl.ds(pl.multiple_of(me * x_local, x_local), x_local), :],
            send_a.at[c, o], recv_a.at[c, o],
        )

    def copy_b(c, o, late):
        to = partner(me, o)
        lane = pl.multiple_of(lax.rem(me, cuts) * LANES, LANES)
        start = near_half if late else far_half
        half = pl.ds(start, near)
        if c < first:
            landing = held.at[c, half, me // cuts, :, pl.ds(lane, LANES)]
        else:
            piece = c % first * levels + me // cuts
            landing = columns.at[first + start // near, piece, :, :, pl.ds(lane, LANES)]
        return move(
            "gx", to,
            waves.at[c, o, half],
            landing,
            send_b.at[late, c, o], recv_b.at[late, c, o],
        )

    def copy_c(c, o):
        to = partner(my, o)
        return move(
            "gy", to, held.at[c, to], columns.at[c, my], send_c.at[c, o], recv_c.at[c, o]
        )

    def copy_d(c, o):
        to = partner(my, o)
        if c < first:
            landing = out.at[:, pl.ds(c * levels, levels), my]
        else:
            landing = out.at[:, first * levels + my, pl.ds(c % first * levels, levels)]
        return move(
            "gy", to,
            spectra.at[c, o],
            landing,
            send_d.at[c, o], recv_d.at[c, o],
        )

    def start_all(copy, c, offsets):
        for o in offsets:
            remote, local = copy(c, o)
            (remote() if o else local()).start()

    def arrive(copy, c, offsets):
        for o in offsets:
            remote, local = copy(c, o)
            if o:
                remote().wait_recv()
            else:
                local().wait()

    def first_b(c, o):
        return copy_b(c, o, 0)

    def late_b(c, o):
        return copy_b(c, o, 1)

    def circle(phases):
        turns = phases.astype(jnp.float32) * (1.0 / nx)
        halves = jnp.floor(2.0 * turns + 0.5)
        angle = (turns - 0.5 * halves) * (2.0 * math.pi)
        sign = 1.0 - 2.0 * halves * (2.0 - halves)
        square = angle * angle
        cos = jnp.full_like(square, 1.0 / math.factorial(12))
        sin = jnp.full_like(square, 1.0 / math.factorial(13))
        for power in range(10, -1, -2):
            flip = -1.0 if power % 4 else 1.0
            cos = cos * square + flip / math.factorial(power)
            sin = sin * square + flip / math.factorial(power + 1)
        return cos * sign, sin * angle * sign

    def make_table(step, carry):
        waves_at = order_column[pl.ds(pl.multiple_of(step * rows, rows), rows), :]
        points = lax.broadcasted_iota(jnp.int32, (rows, x_local), 1)
        near_waves = jnp.concatenate([waves_at] * (x_local // LANES), axis=1)
        near_cos, near_sin = circle(near_waves * points & (nx - 1))
        blocks = lax.broadcasted_iota(jnp.int32, (rows, LANES), 1) * x_local
        far_cos, far_sin = circle(waves_at * blocks & (nx - 1))
        first = pl.multiple_of(2 * step * rows, rows)
        for j in range(gx):
            cos, sin = far_cos[:, j : j + 1], far_sin[:, j : j + 1]
            lanes = slice(j * x_local, (j + 1) * x_local)
            for part, value in enumerate(
                (cos * near_cos - sin * near_sin, -(sin * near_cos + cos * near_sin))
            ):
                at = pl.ds(pl.multiple_of(first + part * rows, rows), rows)
                high, low = split_halves(value)
                x_high[at, lanes] = high
                x_low[at, lanes] = low
        return carry

    def x_stage(c):
        def split_block(j, carry):
            at = pl.ds(pl.multiple_of(j * x_local, x_local), x_local)
            high, low = split_halves(lines[c, at, :])
            split_lines[at, :LANES] = high
            split_lines[at, LANES:] = low
            return carry

        lax.fori_loop(0, gx, split_block, 0)

        def one(step, carry):
            o = gx - 1 - step
            to = partner(me, o)
            at = pl.ds(pl.multiple_of(to * block, block), block)
            main = mxu(x_high[at, :], split_lines[...])
            rest = mxu(x_low[at, :], split_lines[:, :LANES])
            total = main[:, :LANES] + main[:, LANES:] + rest
            waves[c, o] = total.reshape(gy, 2 * rows, LANES)
            remote, local = first_b(c, o)
            pl.when(o != 0)(lambda: remote().start())
            pl.when(o == 0)(lambda: local().start())
            return carry

        lax.fori_loop(0, gx, one, 0)
        start_all(late_b, c, x_order)

    def y_stage(c):
        size = 16
        span = levels * rows
        for level in range(levels):
            for i in range(0, rows, size):
                re = [columns[c, g, level, i : i + size, :] for g in range(4)]
                im = [columns[c, g, level, rows + i : rows + i + size, :] for g in range(4)]
                re_even, re_odd = re[0] + re[2], re[0] - re[2]
                im_even, im_odd = im[0] + im[2], im[0] - im[2]
                re_sum, re_gap = re[1] + re[3], re[1] - re[3]
                im_sum, im_gap = im[1] + im[3], im[1] - im[3]
                legs = (
                    (re_even + re_sum, im_even + im_sum),
                    (re_odd + im_gap, im_odd - re_gap),
                    (re_even - re_sum, im_even - im_sum),
                    (re_odd - im_gap, im_odd + re_gap),
                )
                for r, (a, b) in enumerate(legs):
                    cos = twiddle[r : r + 1, :]
                    sin = twiddle[gy + r : gy + r + 1, :]
                    for part, value in enumerate((a * cos + b * sin, b * cos - a * sin)):
                        at = part * gy * span + r * span + level * rows + i
                        high, low = split_halves(value)
                        z_high[at : at + size, :] = high
                        z_low[at : at + size, :] = low

        def one(step, carry):
            o = turn(step)
            to = partner(my, o)
            table = y_high[to]
            terms = mxu(z_high[...], table) + mxu(z_low[...], table) + mxu(z_high[...], y_low[to])
            half = gy * span
            wide = y_local // gy
            re = terms[:half, :wide] + terms[half:, wide:]
            im = terms[half:, :wide] - terms[:half, wide:]
            whole = jnp.concatenate(
                [
                    jnp.concatenate([piece[r * span : (r + 1) * span] for r in range(gy)], axis=1)
                    for piece in (re, im)
                ],
                axis=0,
            )
            high, low = split_halves(whole)
            ordered = mxu(high, order[...]) + mxu(low, order[...])
            spectra[c, o] = ordered.reshape(2, levels, rows, y_local)
            remote, local = copy_d(c, o)
            pl.when(o != 0)(lambda: remote().start())
            pl.when(o == 0)(lambda: local().start())
            return carry

        lax.fori_loop(0, gy, one, 0)

    barrier = pltpu.get_barrier_semaphore()
    lone = lone_at(me, my)

    def greet(semaphore, axis, target):
        pl.semaphore_signal(
            semaphore, inc=1, device_id={axis: target}, device_id_type=MESH_IDS
        )

    greet(barrier, "gy", partner(my, gy - 1))
    for o in range(1, gy - 1):
        to = partner(my, o)
        pl.when(lone_at(me, to) == 0)(functools.partial(greet, barrier, "gy", to))
    for o in range(1, gx):
        to = partner(me, o)
        pl.when(lone_at(to, my) == 0)(functools.partial(greet, barrier, "gx", to))
    pl.semaphore_wait(barrier, 1 + (1 - lone) * (gx + gy - 3))
    start_all(copy_r, 0, (gy - 1,))

    def release():
        for o in range(1, gy - 1):
            to = partner(my, o)
            pl.when(lone_at(me, to) * (1 - inner_at(my)) == 1)(
                functools.partial(greet, go, "gy", to)
            )
        for o in range(1, gx):
            to = partner(me, o)
            pl.when(lone_at(to, my) == 1)(functools.partial(greet, go, "gx", to))

    pl.when(lone == 0)(release)
    pl.when(lone == 1)(lambda: pl.semaphore_wait(go, gx // 2 + gy // 2))
    start_all(copy_r, 0, y_order[1:])
    start_all(copy_a, 0, x_order)
    tables = [
        pltpu.make_async_copy(src, dst, table_sem.at[i])
        for i, (src, dst) in enumerate(
            (
                (order_rows_in, order_rows),
                (twiddle_in, twiddle),
                (y_high_in, y_high),
                (y_low_in, y_low),
                (order_in, order),
            )
        )
    ]
    for table in tables:
        table.start()
    tables[0].wait()
    for i in range(order_rows.shape[0]):
        row = jnp.broadcast_to(order_rows[i : i + 1, :], (LANES, LANES))
        order_column[i * LANES : (i + 1) * LANES, :] = row.T
    lax.fori_loop(0, x_high.shape[0] // (2 * rows), make_table, 0)
    for table in tables[1:]:
        table.wait()

    def forward(c):
        arrive(first_b, c, x_order)
        start_all(copy_c, c, (3, 2))
        arrive(late_b, c, x_order)
        start_all(copy_c, c, (1, 0))

    def lines_stage(c):
        arrive(copy_a, c, x_order)
        x_stage(c)

    def columns_stage(c):
        arrive(copy_c, c, y_order)
        y_stage(c)

    lines_stage(0)
    start_all(copy_a, 1, x_order)
    forward(0)
    lines_stage(1)
    arrive(copy_r, 0, y_order)
    start_all(copy_a, 2, x_order)
    start_all(copy_a, 3, x_order)
    forward(1)
    columns_stage(0)
    lines_stage(2)
    lines_stage(3)
    columns_stage(1)
    for c in (2, 3):
        arrive(first_b, c, x_order)
        arrive(late_b, c, x_order)
    y_stage(2)
    y_stage(3)

    def sent(copy, c, offsets):
        for o in offsets:
            if o:
                copy(c, o)[0]().wait_send()

    for c in range(chunks):
        arrive(copy_d, c, y_order)
    sent(copy_r, 0, y_order)
    for c in range(chunks):
        for copy in (copy_a, first_b, late_b):
            sent(copy, c, x_order)
        if c < first:
            sent(copy_c, c, y_order)
        sent(copy_d, c, y_order)


def keep_kernel(scale, spectra, kept_mask, out, kept, sems):
    copies = []
    for piece in range(spectra.shape[0]):
        kept[piece] = spectra[piece] * (kept_mask[...].astype(jnp.float32) * scale)
        copies.append(pltpu.make_async_copy(kept.at[piece], out.at[piece], sems.at[piece]))
        copies[-1].start()
    for copy in copies:
        copy.wait()


def stay(value):
    return pltpu.with_memory_space_constraint(value, pltpu.HBM)


def kernel_shards(gx, gy, fields, wave_order, kept_mask):
    stack, x_local, y_local = fields.shape
    nx, ny = x_local * gx, y_local * gy
    levels = gx * LANES // y_local
    chunks = stack // levels
    rows = wave_order.shape[0] // (gx * gy)
    all_rows = 2 * wave_order.shape[0]
    twiddle, y_high, y_low, order = y_tables(y_local, gy)
    order_rows = wave_order.reshape(-1, LANES)
    vmem = pl.BlockSpec(memory_space=pltpu.VMEM)
    anywhere = pl.BlockSpec(memory_space=pl.ANY)
    hbm = pl.BlockSpec(memory_space=pl.ANY)
    z_rows = 2 * gy * levels * rows
    spectra = pl.pallas_call(
        functools.partial(exchange_kernel, gx, gy, levels, chunks),
        out_shape=pltpu.VMEM((2, stack, gy, rows, y_local), jnp.float32),
        in_specs=[hbm] * 6,
        out_specs=anywhere,
        scratch_shapes=[
            pltpu.VMEM(order_rows.shape, jnp.int32),
            pltpu.VMEM(twiddle.shape, jnp.float32),
            pltpu.VMEM((wave_order.shape[0], LANES), jnp.int32),
            pltpu.VMEM((all_rows, nx), jnp.bfloat16),
            pltpu.VMEM((all_rows, nx), jnp.bfloat16),
            pltpu.VMEM((chunks, nx, LANES), jnp.float32),
            pltpu.VMEM((nx, 2 * LANES), jnp.bfloat16),
            pltpu.VMEM((chunks, gx, gy, 2 * rows, LANES), jnp.float32),
            pltpu.VMEM((chunks, gy, levels, 2 * rows, y_local), jnp.float32),
            pltpu.VMEM((chunks, gy, levels, 2 * rows, y_local), jnp.float32),
            pltpu.VMEM((z_rows, y_local), jnp.bfloat16),
            pltpu.VMEM((z_rows, y_local), jnp.bfloat16),
            pltpu.VMEM((chunks, gy, 2, levels, rows, y_local), jnp.float32),
            pltpu.VMEM(y_high.shape, jnp.bfloat16),
            pltpu.VMEM(y_low.shape, jnp.bfloat16),
            pltpu.VMEM(order.shape, jnp.bfloat16),
            pltpu.VMEM((gy, x_local, y_local), jnp.float32),
        ]
        + [pltpu.SemaphoreType.DMA((1, gy))] * 2
        + [pltpu.SemaphoreType.DMA((chunks, gx))] * 2
        + [pltpu.SemaphoreType.DMA((2, chunks, gx))] * 2
        + [pltpu.SemaphoreType.DMA((chunks, gy))] * 4
        + [pltpu.SemaphoreType.DMA((5,)), pltpu.SemaphoreType.REGULAR],
        compiler_params=pltpu.CompilerParams(
            collective_id=0, has_side_effects=True, vmem_limit_bytes=58 * 1024 * 1024
        ),
        name="exchange",
    )(*map(stay, (fields, order_rows, twiddle, y_high, y_low, order)))
    pieces = 2 * stack
    kept = pl.pallas_call(
        functools.partial(keep_kernel, 1.0 / math.sqrt(nx * ny)),
        out_shape=jax.ShapeDtypeStruct((pieces, gy * rows, y_local), jnp.float32),
        in_specs=[vmem, vmem],
        out_specs=anywhere,
        scratch_shapes=[
            pltpu.VMEM((pieces, gy * rows, y_local), jnp.float32),
            pltpu.SemaphoreType.DMA((pieces,)),
        ],
        compiler_params=pltpu.CompilerParams(vmem_limit_bytes=6 * 1024 * 1024),
        name="keep",
    )(spectra.reshape(pieces, gy * rows, y_local), kept_mask)
    return kept.reshape(2, stack, gy * rows, y_local)


def kernel_fits(gx, gy):
    y_local, x_local = NY // gy, NX // gx
    if gx != 8 or gy != 4 or NX & (NX - 1) or y_local % (4 * LANES) or x_local % LANES or gx * LANES % y_local:
        return False
    levels = gx * LANES // y_local
    return STACK == 4 * levels == 2 * gy and KX % (gx * gy * 16) == 0


def solution(mesh):
    gx, gy = mesh.shape["gx"], mesh.shape["gy"]
    body = functools.partial(kernel_shards, gx, gy) if kernel_fits(gx, gy) else shards
    return jax.shard_map(
        body,
        mesh=mesh,
        in_specs=(P(None, "gx", "gy"), P(), P("gx", "gy")),
        out_specs=P(None, None, "gx", "gy"),
        check_vma=False,
    )
```

```python
import functools
import math

import jax
import jax.numpy as jnp
import numpy as np
from jax import lax
from jax.experimental import pallas as pl
from jax.experimental.pallas import tpu as pltpu
from jax.sharding import PartitionSpec as P

NX = 2048
NY = 2048
STACK = 8
KX = 1024


def wave_angles(wave_ids, points, period):
    phases = wave_ids[:, None] * points[None, :] % period
    angles = phases.astype(jnp.float32) * (2.0 * math.pi / period)
    return (jnp.cos(angles), jnp.sin(angles))


def x_terms(cos_table, sin_table, values):
    stack_count, x_count, y_count = values.shape
    waves = cos_table.shape[0]
    table = jnp.concatenate([cos_table, -sin_table], axis=0)
    flat = jnp.transpose(values, (1, 0, 2)).reshape(x_count, stack_count * y_count)
    product = jnp.dot(
        table, flat, precision=lax.Precision.HIGHEST, preferred_element_type=jnp.float32
    )
    product = product.reshape(2, waves, stack_count, y_count)
    return jnp.transpose(product, (1, 0, 2, 3))


def y_terms(cos_table, sin_table, spectra):
    rows, parts, stack_count, y_count = spectra.shape
    waves = cos_table.shape[0]
    table = jnp.concatenate([cos_table, sin_table], axis=0)
    flat = spectra.reshape(rows * parts * stack_count, y_count)
    product = jnp.dot(
        flat, table.T, precision=lax.Precision.HIGHEST, preferred_element_type=jnp.float32
    )
    product = product.reshape(rows, parts, stack_count, 2, waves)
    real_part = product[:, 0, :, 0] + product[:, 1, :, 1]
    imag_part = product[:, 1, :, 0] - product[:, 0, :, 1]
    return jnp.stack([real_part, imag_part], axis=1)


def shards(fields, wave_order, kept_mask):
    x_every = jnp.arange(NX, dtype=jnp.int32)
    x_cos, x_sin = wave_angles(wave_order, x_every, NX)
    partial_terms = x_terms(
        x_cos, x_sin, lax.all_to_all(fields, "gx", split_axis=2, concat_axis=1, tiled=True)
    )
    spectra = lax.all_to_all(partial_terms, "gx", split_axis=0, concat_axis=3, tiled=True)
    y_every = jnp.arange(NY, dtype=jnp.int32)
    y_cos, y_sin = wave_angles(y_every, y_every, NY)
    y_spectra = y_terms(
        y_cos, y_sin, lax.all_to_all(spectra, "gy", split_axis=0, concat_axis=3, tiled=True)
    )
    result = lax.all_to_all(y_spectra, "gy", split_axis=3, concat_axis=0, tiled=True)
    weight = kept_mask.astype(jnp.float32) * (1.0 / math.sqrt(NX * NY))
    arranged = jnp.transpose(result, (1, 2, 0, 3)) * weight[None, None]
    return arranged


LANES = 128
MESH_IDS = pl.DeviceIdType.MESH


def split_halves(values):
    high = values.astype(jnp.bfloat16)
    return high, (values - high.astype(jnp.float32)).astype(jnp.bfloat16)


def table_halves(table):
    high = table.astype(jnp.bfloat16)
    low = (table - high.astype(np.float64)).astype(jnp.bfloat16)
    return jnp.asarray(high), jnp.asarray(low)


def mxu(left, right):
    return jnp.dot(left, right, preferred_element_type=jnp.float32)


def y_tables(y_local, parts):
    points = np.arange(y_local)
    period = y_local * parts
    turns = np.arange(parts)[:, None] * points[None, :] % period * (2.0 * np.pi / period)
    twiddle = jnp.asarray(np.concatenate([np.cos(turns), np.sin(turns)]), jnp.float32)
    angles = points[:, None] * points[None, :] % y_local * (2.0 * np.pi / y_local)
    cos = np.cos(angles).reshape(y_local, parts, -1)
    sin = np.sin(angles).reshape(y_local, parts, -1)
    both = np.concatenate([cos, sin], axis=2).transpose(1, 0, 2)
    high, low = table_halves(both)
    wide = y_local // parts
    order = np.zeros((y_local, y_local), np.float32)
    for residue in range(parts):
        order[residue * wide + np.arange(wide), parts * np.arange(wide) + residue] = 1.0
    return twiddle, high, low, jnp.asarray(order, jnp.bfloat16)


def exchange_kernel(
    gx, gy, levels, chunks,
    fields, order_rows_in, twiddle_in, y_high_in, y_low_in, order_in, out,
    order_rows, twiddle, order_column, x_high, x_low, lines, split_lines, waves, held, columns, z_high, z_low, spectra,
    y_high, y_low, order, whole_y,
    send_r, recv_r, send_a, recv_a, send_b, recv_b, send_c, recv_c, send_d, recv_d, table_sem, go,
):
    me = lax.axis_index("gx")
    my = lax.axis_index("gy")
    x_local = fields.shape[1]
    y_local = fields.shape[2]
    rows = out.shape[3]
    first = chunks // 2
    cuts = y_local // LANES
    block = 2 * rows * gy
    nx = gx * x_local
    near = gy // 2
    far_half = (1 - my // near) * near
    near_half = my // near * near
    x_order = (6, 7, 4, 2, 5, 3, 1, 0)
    y_order = (3, 2, 1, 0)

    def partner(index, o):
        total = 0
        for bit in (1, 2, 4):
            total = total + bit * lax.rem(index // bit + o // bit, 2)
        return total

    def inner_at(y_index):
        return lax.rem(y_index + 1, gy) // 2

    def lone_at(x_index, y_index):
        return inner_at(y_index) * lax.rem(x_index, 2)

    def turn(step):
        inner = inner_at(my)
        is_first = (3 - step) // 3
        is_second = lax.rem(step, 2) * ((3 - step) // 2)
        is_third = step // 2 * ((4 - step) // 2)
        return is_first * (1 + inner) + is_second * 3 + is_third * (2 - inner)

    lone = lone_at(me, my)

    def move(axis, target, src, dst, send, recv):
        def remote():
            return pltpu.make_async_remote_copy(
                src_ref=src, dst_ref=dst, send_sem=send, recv_sem=recv,
                device_id={axis: target}, device_id_type=MESH_IDS,
            )

        def local():
            return pltpu.make_async_copy(src, dst, recv)

        return remote, local

    def copy_r(c, o):
        to = partner(my, o)
        return move(
            "gy", to, fields.at[first * levels + to], whole_y.at[my],
            send_r.at[c, o], recv_r.at[c, o],
        )

    def copy_a(c, o):
        to = partner(me, o)
        level = c % first * levels + to // cuts
        source = fields if c < first else whole_y
        lane = pl.multiple_of(lax.rem(to, cuts) * LANES, LANES)
        return move(
            "gx", to,
            source.at[level, :, pl.ds(lane, LANES)],
            lines.at[c, pl.ds(pl.multiple_of(me * x_local, x_local), x_local), :],
            send_a.at[c, o], recv_a.at[c, o],
        )

    def copy_b(c, o, late):
        to = partner(me, o)
        lane = pl.multiple_of(lax.rem(me, cuts) * LANES, LANES)
        start = near_half if late else far_half
        half = pl.ds(start, near)
        if c < first:
            landing = held.at[c, half, me // cuts, :, pl.ds(lane, LANES)]
        else:
            piece = c % first * levels + me // cuts
            landing = columns.at[first + start // near, piece, :, :, pl.ds(lane, LANES)]
        return move(
            "gx", to,
            waves.at[c, o, half],
            landing,
            send_b.at[late, c, o], recv_b.at[late, c, o],
        )

    def copy_c(c, o):
        to = partner(my, o)
        return move(
            "gy", to, held.at[c, to], columns.at[c, my], send_c.at[c, o], recv_c.at[c, o]
        )

    def copy_d(c, o):
        to = partner(my, o)
        if c < first:
            landing = out.at[:, pl.ds(c * levels, levels), my]
        else:
            landing = out.at[:, first * levels + my, pl.ds(c % first * levels, levels)]
        return move(
            "gy", to,
            spectra.at[c, o],
            landing,
            send_d.at[c, o], recv_d.at[c, o],
        )

    def start_all(copy, c, offsets):
        for o in offsets:
            remote, local = copy(c, o)
            (remote() if o else local()).start()

    def arrive(copy, c, offsets):
        for o in offsets:
            remote, local = copy(c, o)
            if o:
                remote().wait_recv()
            else:
                local().wait()

    def first_b(c, o):
        return copy_b(c, o, 0)

    def late_b(c, o):
        return copy_b(c, o, 1)

    def circle(phases):
        turns = phases.astype(jnp.float32) * (1.0 / nx)
        halves = jnp.floor(2.0 * turns + 0.5)
        angle = (turns - 0.5 * halves) * (2.0 * math.pi)
        sign = 1.0 - 2.0 * halves * (2.0 - halves)
        square = angle * angle
        cos = jnp.full_like(square, 1.0 / math.factorial(12))
        sin = jnp.full_like(square, 1.0 / math.factorial(13))
        for power in range(10, -1, -2):
            flip = -1.0 if power % 4 else 1.0
            cos = cos * square + flip / math.factorial(power)
            sin = sin * square + flip / math.factorial(power + 1)
        return cos * sign, sin * angle * sign

    def make_table(step, carry):
        waves_at = order_column[pl.ds(pl.multiple_of(step * rows, rows), rows), :]
        points = lax.broadcasted_iota(jnp.int32, (rows, x_local), 1)
        near_waves = jnp.concatenate([waves_at] * (x_local // LANES), axis=1)
        near_cos, near_sin = circle(near_waves * points & (nx - 1))
        blocks = lax.broadcasted_iota(jnp.int32, (rows, LANES), 1) * x_local
        far_cos, far_sin = circle(waves_at * blocks & (nx - 1))
        first = pl.multiple_of(2 * step * rows, rows)
        for j in range(gx):
            cos, sin = far_cos[:, j : j + 1], far_sin[:, j : j + 1]
            lanes = slice(j * x_local, (j + 1) * x_local)
            for part, value in enumerate(
                (cos * near_cos - sin * near_sin, -(sin * near_cos + cos * near_sin))
            ):
                at = pl.ds(pl.multiple_of(first + part * rows, rows), rows)
                high, low = split_halves(value)
                x_high[at, lanes] = high
                x_low[at, lanes] = low
        return carry

    def x_stage(c):
        def split_block(j, carry):
            at = pl.ds(pl.multiple_of(j * x_local, x_local), x_local)
            high, low = split_halves(lines[c, at, :])
            split_lines[at, :LANES] = high
            split_lines[at, LANES:] = low
            return carry

        lax.fori_loop(0, gx, split_block, 0)

        def one(step, carry):
            o = gx - 1 - step
            to = partner(me, o)
            at = pl.ds(pl.multiple_of(to * block, block), block)
            main = mxu(x_high[at, :], split_lines[...])
            rest = mxu(x_low[at, :], split_lines[:, :LANES])
            total = main[:, :LANES] + main[:, LANES:] + rest
            waves[c, o] = total.reshape(gy, 2 * rows, LANES)
            remote, local = first_b(c, o)
            pl.when(o != 0)(lambda: remote().start())
            pl.when(o == 0)(lambda: local().start())
            return carry

        lax.fori_loop(0, gx, one, 0)
        start_all(late_b, c, x_order)

    def y_stage(c):
        size = 16
        span = levels * rows
        for level in range(levels):
            for i in range(0, rows, size):
                re = [columns[c, g, level, i : i + size, :] for g in range(4)]
                im = [columns[c, g, level, rows + i : rows + i + size, :] for g in range(4)]
                re_even, re_odd = re[0] + re[2], re[0] - re[2]
                im_even, im_odd = im[0] + im[2], im[0] - im[2]
                re_sum, re_gap = re[1] + re[3], re[1] - re[3]
                im_sum, im_gap = im[1] + im[3], im[1] - im[3]
                legs = (
                    (re_even + re_sum, im_even + im_sum),
                    (re_odd + im_gap, im_odd - re_gap),
                    (re_even - re_sum, im_even - im_sum),
                    (re_odd - im_gap, im_odd + re_gap),
                )
                for r, (a, b) in enumerate(legs):
                    cos = twiddle[r : r + 1, :]
                    sin = twiddle[gy + r : gy + r + 1, :]
                    for part, value in enumerate((a * cos + b * sin, b * cos - a * sin)):
                        at = part * gy * span + r * span + level * rows + i
                        high, low = split_halves(value)
                        z_high[at : at + size, :] = high
                        z_low[at : at + size, :] = low

        def one(step, carry):
            o = turn(step)
            to = partner(my, o)
            table = y_high[to]
            terms = mxu(z_high[...], table) + mxu(z_low[...], table) + mxu(z_high[...], y_low[to])
            half = gy * span
            wide = y_local // gy
            re = terms[:half, :wide] + terms[half:, wide:]
            im = terms[half:, :wide] - terms[:half, wide:]
            whole = jnp.concatenate(
                [
                    jnp.concatenate([piece[r * span : (r + 1) * span] for r in range(gy)], axis=1)
                    for piece in (re, im)
                ],
                axis=0,
            )
            high, low = split_halves(whole)
            ordered = mxu(high, order[...]) + mxu(low, order[...])
            spectra[c, o] = ordered.reshape(2, levels, rows, y_local)
            remote, local = copy_d(c, o)
            now = lone * (o // 2) == 0 if c in (2, 3) else o >= 0
            pl.when(jnp.logical_and(o != 0, now))(lambda: remote().start())
            pl.when(o == 0)(lambda: local().start())
            return carry

        lax.fori_loop(0, gy, one, 0)

    barrier = pltpu.get_barrier_semaphore()
    def greet(semaphore, axis, target):
        pl.semaphore_signal(
            semaphore, inc=1, device_id={axis: target}, device_id_type=MESH_IDS
        )

    greet(barrier, "gy", partner(my, gy - 1))
    for o in range(1, gy - 1):
        to = partner(my, o)
        pl.when(lone_at(me, to) == 0)(functools.partial(greet, barrier, "gy", to))
    for o in range(1, gx):
        to = partner(me, o)
        pl.when(lone_at(to, my) == 0)(functools.partial(greet, barrier, "gx", to))
    pl.semaphore_wait(barrier, 1 + (1 - lone) * (gx + gy - 3))
    start_all(copy_r, 0, (gy - 1,))

    def release():
        for o in range(1, gy - 1):
            to = partner(my, o)
            pl.when(lone_at(me, to) * (1 - inner_at(my)) == 1)(
                functools.partial(greet, go, "gy", to)
            )
        for o in range(1, gx):
            to = partner(me, o)
            pl.when(lone_at(to, my) == 1)(functools.partial(greet, go, "gx", to))

    pl.when(lone == 0)(release)
    pl.when(lone == 1)(lambda: pl.semaphore_wait(go, gx // 2 + gy // 2))
    start_all(copy_r, 0, y_order[1:])
    start_all(copy_a, 0, x_order)
    tables = [
        pltpu.make_async_copy(src, dst, table_sem.at[i])
        for i, (src, dst) in enumerate(
            (
                (order_rows_in, order_rows),
                (twiddle_in, twiddle),
                (y_high_in, y_high),
                (y_low_in, y_low),
                (order_in, order),
            )
        )
    ]
    for table in tables:
        table.start()
    tables[0].wait()
    for i in range(order_rows.shape[0]):
        row = jnp.broadcast_to(order_rows[i : i + 1, :], (LANES, LANES))
        order_column[i * LANES : (i + 1) * LANES, :] = row.T
    lax.fori_loop(0, x_high.shape[0] // (2 * rows), make_table, 0)
    for table in tables[1:]:
        table.wait()

    def forward(c):
        arrive(first_b, c, x_order)
        start_all(copy_c, c, (3, 2))
        arrive(late_b, c, x_order)
        start_all(copy_c, c, (1, 0))

    def lines_stage(c):
        arrive(copy_a, c, x_order)
        x_stage(c)

    def columns_stage(c):
        arrive(copy_c, c, y_order)
        y_stage(c)

    lines_stage(0)
    start_all(copy_a, 1, x_order)
    forward(0)
    lines_stage(1)
    arrive(copy_r, 0, y_order)
    start_all(copy_a, 2, x_order)
    start_all(copy_a, 3, x_order)
    forward(1)
    columns_stage(0)
    lines_stage(2)
    lines_stage(3)
    columns_stage(1)
    for c in (2, 3):
        arrive(first_b, c, x_order)
        arrive(late_b, c, x_order)
    y_stage(2)
    y_stage(3)

    def yielding():
        copy_d(1, 3)[0]().wait_send()
        copy_d(2, 2)[0]().start()
        copy_d(2, 2)[0]().wait_send()
        copy_d(2, 3)[0]().start()
        copy_d(3, 2)[0]().start()
        copy_d(3, 3)[0]().start()

    pl.when(lone == 1)(yielding)

    def sent(copy, c, offsets):
        for o in offsets:
            if o:
                copy(c, o)[0]().wait_send()

    for c in range(chunks):
        arrive(copy_d, c, y_order)
    sent(copy_r, 0, y_order)
    for c in range(chunks):
        for copy in (copy_a, first_b, late_b):
            sent(copy, c, x_order)
        if c < first:
            sent(copy_c, c, y_order)
        for o in (1, 2, 3):
            if (c, o) in ((1, 3), (2, 2)):
                pl.when(lone == 0)(copy_d(c, o)[0]().wait_send)
            else:
                sent(copy_d, c, (o,))


def keep_kernel(scale, spectra, kept_mask, out, kept, sems):
    copies = []
    for piece in range(spectra.shape[0]):
        kept[piece] = spectra[piece] * (kept_mask[...].astype(jnp.float32) * scale)
        copies.append(pltpu.make_async_copy(kept.at[piece], out.at[piece], sems.at[piece]))
        copies[-1].start()
    for copy in copies:
        copy.wait()


def stay(value):
    return pltpu.with_memory_space_constraint(value, pltpu.HBM)


def kernel_shards(gx, gy, fields, wave_order, kept_mask):
    stack, x_local, y_local = fields.shape
    nx, ny = x_local * gx, y_local * gy
    levels = gx * LANES // y_local
    chunks = stack // levels
    rows = wave_order.shape[0] // (gx * gy)
    all_rows = 2 * wave_order.shape[0]
    twiddle, y_high, y_low, order = y_tables(y_local, gy)
    order_rows = wave_order.reshape(-1, LANES)
    vmem = pl.BlockSpec(memory_space=pltpu.VMEM)
    anywhere = pl.BlockSpec(memory_space=pl.ANY)
    hbm = pl.BlockSpec(memory_space=pl.ANY)
    z_rows = 2 * gy * levels * rows
    spectra = pl.pallas_call(
        functools.partial(exchange_kernel, gx, gy, levels, chunks),
        out_shape=pltpu.VMEM((2, stack, gy, rows, y_local), jnp.float32),
        in_specs=[hbm] * 6,
        out_specs=anywhere,
        scratch_shapes=[
            pltpu.VMEM(order_rows.shape, jnp.int32),
            pltpu.VMEM(twiddle.shape, jnp.float32),
            pltpu.VMEM((wave_order.shape[0], LANES), jnp.int32),
            pltpu.VMEM((all_rows, nx), jnp.bfloat16),
            pltpu.VMEM((all_rows, nx), jnp.bfloat16),
            pltpu.VMEM((chunks, nx, LANES), jnp.float32),
            pltpu.VMEM((nx, 2 * LANES), jnp.bfloat16),
            pltpu.VMEM((chunks, gx, gy, 2 * rows, LANES), jnp.float32),
            pltpu.VMEM((chunks, gy, levels, 2 * rows, y_local), jnp.float32),
            pltpu.VMEM((chunks, gy, levels, 2 * rows, y_local), jnp.float32),
            pltpu.VMEM((z_rows, y_local), jnp.bfloat16),
            pltpu.VMEM((z_rows, y_local), jnp.bfloat16),
            pltpu.VMEM((chunks, gy, 2, levels, rows, y_local), jnp.float32),
            pltpu.VMEM(y_high.shape, jnp.bfloat16),
            pltpu.VMEM(y_low.shape, jnp.bfloat16),
            pltpu.VMEM(order.shape, jnp.bfloat16),
            pltpu.VMEM((gy, x_local, y_local), jnp.float32),
        ]
        + [pltpu.SemaphoreType.DMA((1, gy))] * 2
        + [pltpu.SemaphoreType.DMA((chunks, gx))] * 2
        + [pltpu.SemaphoreType.DMA((2, chunks, gx))] * 2
        + [pltpu.SemaphoreType.DMA((chunks, gy))] * 4
        + [pltpu.SemaphoreType.DMA((5,)), pltpu.SemaphoreType.REGULAR],
        compiler_params=pltpu.CompilerParams(
            collective_id=0, has_side_effects=True, vmem_limit_bytes=58 * 1024 * 1024
        ),
        name="exchange",
    )(*map(stay, (fields, order_rows, twiddle, y_high, y_low, order)))
    pieces = 2 * stack
    kept = pl.pallas_call(
        functools.partial(keep_kernel, 1.0 / math.sqrt(nx * ny)),
        out_shape=jax.ShapeDtypeStruct((pieces, gy * rows, y_local), jnp.float32),
        in_specs=[vmem, vmem],
        out_specs=anywhere,
        scratch_shapes=[
            pltpu.VMEM((pieces, gy * rows, y_local), jnp.float32),
            pltpu.SemaphoreType.DMA((pieces,)),
        ],
        compiler_params=pltpu.CompilerParams(vmem_limit_bytes=6 * 1024 * 1024),
        name="keep",
    )(spectra.reshape(pieces, gy * rows, y_local), kept_mask)
    return kept.reshape(2, stack, gy * rows, y_local)


def kernel_fits(gx, gy):
    y_local, x_local = NY // gy, NX // gx
    if gx != 8 or gy != 4 or NX & (NX - 1) or y_local % (4 * LANES) or x_local % LANES or gx * LANES % y_local:
        return False
    levels = gx * LANES // y_local
    return STACK == 4 * levels == 2 * gy and KX % (gx * gy * 16) == 0


def solution(mesh):
    gx, gy = mesh.shape["gx"], mesh.shape["gy"]
    body = functools.partial(kernel_shards, gx, gy) if kernel_fits(gx, gy) else shards
    return jax.shard_map(
        body,
        mesh=mesh,
        in_specs=(P(None, "gx", "gy"), P(), P("gx", "gy")),
        out_specs=P(None, None, "gx", "gy"),
        check_vma=False,
    )
```

```python
import functools
import math

import jax
import jax.numpy as jnp
import numpy as np
from jax import lax
from jax.experimental import pallas as pl
from jax.experimental.pallas import tpu as pltpu
from jax.sharding import PartitionSpec as P

NX = 2048
NY = 2048
STACK = 8
KX = 1024


def wave_angles(wave_ids, points, period):
    phases = wave_ids[:, None] * points[None, :] % period
    angles = phases.astype(jnp.float32) * (2.0 * math.pi / period)
    return (jnp.cos(angles), jnp.sin(angles))


def x_terms(cos_table, sin_table, values):
    stack_count, x_count, y_count = values.shape
    waves = cos_table.shape[0]
    table = jnp.concatenate([cos_table, -sin_table], axis=0)
    flat = jnp.transpose(values, (1, 0, 2)).reshape(x_count, stack_count * y_count)
    product = jnp.dot(
        table, flat, precision=lax.Precision.HIGHEST, preferred_element_type=jnp.float32
    )
    product = product.reshape(2, waves, stack_count, y_count)
    return jnp.transpose(product, (1, 0, 2, 3))


def y_terms(cos_table, sin_table, spectra):
    rows, parts, stack_count, y_count = spectra.shape
    waves = cos_table.shape[0]
    table = jnp.concatenate([cos_table, sin_table], axis=0)
    flat = spectra.reshape(rows * parts * stack_count, y_count)
    product = jnp.dot(
        flat, table.T, precision=lax.Precision.HIGHEST, preferred_element_type=jnp.float32
    )
    product = product.reshape(rows, parts, stack_count, 2, waves)
    real_part = product[:, 0, :, 0] + product[:, 1, :, 1]
    imag_part = product[:, 1, :, 0] - product[:, 0, :, 1]
    return jnp.stack([real_part, imag_part], axis=1)


def shards(fields, wave_order, kept_mask):
    x_every = jnp.arange(NX, dtype=jnp.int32)
    x_cos, x_sin = wave_angles(wave_order, x_every, NX)
    partial_terms = x_terms(
        x_cos, x_sin, lax.all_to_all(fields, "gx", split_axis=2, concat_axis=1, tiled=True)
    )
    spectra = lax.all_to_all(partial_terms, "gx", split_axis=0, concat_axis=3, tiled=True)
    y_every = jnp.arange(NY, dtype=jnp.int32)
    y_cos, y_sin = wave_angles(y_every, y_every, NY)
    y_spectra = y_terms(
        y_cos, y_sin, lax.all_to_all(spectra, "gy", split_axis=0, concat_axis=3, tiled=True)
    )
    result = lax.all_to_all(y_spectra, "gy", split_axis=3, concat_axis=0, tiled=True)
    weight = kept_mask.astype(jnp.float32) * (1.0 / math.sqrt(NX * NY))
    arranged = jnp.transpose(result, (1, 2, 0, 3)) * weight[None, None]
    return arranged


LANES = 128
MESH_IDS = pl.DeviceIdType.MESH


def split_halves(values):
    high = values.astype(jnp.bfloat16)
    return high, (values - high.astype(jnp.float32)).astype(jnp.bfloat16)


def table_halves(table):
    high = table.astype(jnp.bfloat16)
    low = (table - high.astype(np.float64)).astype(jnp.bfloat16)
    return jnp.asarray(high), jnp.asarray(low)


def mxu(left, right):
    return jnp.dot(left, right, preferred_element_type=jnp.float32)


def y_tables(y_local, parts):
    points = np.arange(y_local)
    period = y_local * parts
    turns = np.arange(parts)[:, None] * points[None, :] % period * (2.0 * np.pi / period)
    twiddle = jnp.asarray(np.concatenate([np.cos(turns), np.sin(turns)]), jnp.float32)
    angles = points[:, None] * points[None, :] % y_local * (2.0 * np.pi / y_local)
    cos = np.cos(angles).reshape(y_local, parts, -1)
    sin = np.sin(angles).reshape(y_local, parts, -1)
    both = np.concatenate([cos, sin], axis=2).transpose(1, 0, 2)
    high, low = table_halves(both)
    wide = y_local // parts
    order = np.zeros((y_local, y_local), np.float32)
    for residue in range(parts):
        order[residue * wide + np.arange(wide), parts * np.arange(wide) + residue] = 1.0
    return twiddle, high, low, jnp.asarray(order, jnp.bfloat16)


def exchange_kernel(
    gx, gy, levels, chunks,
    fields, order_rows_in, twiddle_in, y_high_in, y_low_in, order_in, out,
    staged, order_rows, twiddle, order_column, x_high, x_low, lines, split_lines, waves, held, columns, z_high, z_low, spectra,
    y_high, y_low, order, whole_y,
    send_r, recv_r, send_a, recv_a, send_b, recv_b, send_c, recv_c, send_d, recv_d, table_sem, stage_sem, go,
):
    me = lax.axis_index("gx")
    my = lax.axis_index("gy")
    x_local = fields.shape[1]
    y_local = fields.shape[2]
    rows = out.shape[3]
    first = chunks // 2
    cuts = y_local // LANES
    block = 2 * rows * gy
    nx = gx * x_local
    near = gy // 2
    far_half = (1 - my // near) * near
    near_half = my // near * near
    x_order = (6, 7, 4, 2, 5, 3, 1, 0)
    y_order = (3, 2, 1, 0)

    def partner(index, o):
        total = 0
        for bit in (1, 2, 4):
            total = total + bit * lax.rem(index // bit + o // bit, 2)
        return total

    def inner_at(y_index):
        return lax.rem(y_index + 1, gy) // 2

    def lone_at(x_index, y_index):
        return inner_at(y_index) * lax.rem(x_index, 2)

    def turn(step):
        inner = inner_at(my)
        is_first = (3 - step) // 3
        is_second = lax.rem(step, 2) * ((3 - step) // 2)
        is_third = step // 2 * ((4 - step) // 2)
        return is_first * (1 + inner) + is_second * 3 + is_third * (2 - inner)

    def move(axis, target, src, dst, send, recv):
        def remote():
            return pltpu.make_async_remote_copy(
                src_ref=src, dst_ref=dst, send_sem=send, recv_sem=recv,
                device_id={axis: target}, device_id_type=MESH_IDS,
            )

        def local():
            return pltpu.make_async_copy(src, dst, recv)

        return remote, local

    def copy_r(c, o):
        to = partner(my, o)
        return move(
            "gy", to, staged.at[o - 1] if o in (1, 2) else fields.at[first * levels + to],
            whole_y.at[my],
            send_r.at[c, o], recv_r.at[c, o],
        )

    def copy_a(c, o):
        to = partner(me, o)
        level = c % first * levels + to // cuts
        source = fields if c < first else whole_y
        lane = pl.multiple_of(lax.rem(to, cuts) * LANES, LANES)
        return move(
            "gx", to,
            source.at[level, :, pl.ds(lane, LANES)],
            lines.at[c, pl.ds(pl.multiple_of(me * x_local, x_local), x_local), :],
            send_a.at[c, o], recv_a.at[c, o],
        )

    def copy_b(c, o, late):
        to = partner(me, o)
        lane = pl.multiple_of(lax.rem(me, cuts) * LANES, LANES)
        start = near_half if late else far_half
        half = pl.ds(start, near)
        if c < first:
            landing = held.at[c, half, me // cuts, :, pl.ds(lane, LANES)]
        else:
            piece = c % first * levels + me // cuts
            landing = columns.at[first + start // near, piece, :, :, pl.ds(lane, LANES)]
        return move(
            "gx", to,
            waves.at[c, o, half],
            landing,
            send_b.at[late, c, o], recv_b.at[late, c, o],
        )

    def copy_c(c, o):
        to = partner(my, o)
        return move(
            "gy", to, held.at[c, to], columns.at[c, my], send_c.at[c, o], recv_c.at[c, o]
        )

    def copy_d(c, o):
        to = partner(my, o)
        if c < first:
            landing = out.at[:, pl.ds(c * levels, levels), my]
        else:
            landing = out.at[:, first * levels + my, pl.ds(c % first * levels, levels)]
        return move(
            "gy", to,
            spectra.at[c, o],
            landing,
            send_d.at[c, o], recv_d.at[c, o],
        )

    def start_all(copy, c, offsets):
        for o in offsets:
            remote, local = copy(c, o)
            (remote() if o else local()).start()

    def arrive(copy, c, offsets):
        for o in offsets:
            remote, local = copy(c, o)
            if o:
                remote().wait_recv()
            else:
                local().wait()

    def first_b(c, o):
        return copy_b(c, o, 0)

    def late_b(c, o):
        return copy_b(c, o, 1)

    def circle(phases):
        turns = phases.astype(jnp.float32) * (1.0 / nx)
        halves = jnp.floor(2.0 * turns + 0.5)
        angle = (turns - 0.5 * halves) * (2.0 * math.pi)
        sign = 1.0 - 2.0 * halves * (2.0 - halves)
        square = angle * angle
        cos = jnp.full_like(square, 1.0 / math.factorial(12))
        sin = jnp.full_like(square, 1.0 / math.factorial(13))
        for power in range(10, -1, -2):
            flip = -1.0 if power % 4 else 1.0
            cos = cos * square + flip / math.factorial(power)
            sin = sin * square + flip / math.factorial(power + 1)
        return cos * sign, sin * angle * sign

    def make_table(step, carry):
        waves_at = order_column[pl.ds(pl.multiple_of(step * rows, rows), rows), :]
        points = lax.broadcasted_iota(jnp.int32, (rows, x_local), 1)
        near_waves = jnp.concatenate([waves_at] * (x_local // LANES), axis=1)
        near_cos, near_sin = circle(near_waves * points & (nx - 1))
        blocks = lax.broadcasted_iota(jnp.int32, (rows, LANES), 1) * x_local
        far_cos, far_sin = circle(waves_at * blocks & (nx - 1))
        first = pl.multiple_of(2 * step * rows, rows)
        for j in range(gx):
            cos, sin = far_cos[:, j : j + 1], far_sin[:, j : j + 1]
            lanes = slice(j * x_local, (j + 1) * x_local)
            for part, value in enumerate(
                (cos * near_cos - sin * near_sin, -(sin * near_cos + cos * near_sin))
            ):
                at = pl.ds(pl.multiple_of(first + part * rows, rows), rows)
                high, low = split_halves(value)
                x_high[at, lanes] = high
                x_low[at, lanes] = low
        return carry

    def x_stage(c):
        def split_block(j, carry):
            at = pl.ds(pl.multiple_of(j * x_local, x_local), x_local)
            high, low = split_halves(lines[c, at, :])
            split_lines[at, :LANES] = high
            split_lines[at, LANES:] = low
            return carry

        lax.fori_loop(0, gx, split_block, 0)

        def one(step, carry):
            o = gx - 1 - step
            to = partner(me, o)
            at = pl.ds(pl.multiple_of(to * block, block), block)
            main = mxu(x_high[at, :], split_lines[...])
            rest = mxu(x_low[at, :], split_lines[:, :LANES])
            total = main[:, :LANES] + main[:, LANES:] + rest
            waves[c, o] = total.reshape(gy, 2 * rows, LANES)
            remote, local = first_b(c, o)
            pl.when(o != 0)(lambda: remote().start())
            pl.when(o == 0)(lambda: local().start())
            return carry

        lax.fori_loop(0, gx, one, 0)
        start_all(late_b, c, x_order)

    def y_stage(c):
        size = 16
        span = levels * rows
        for level in range(levels):
            for i in range(0, rows, size):
                re = [columns[c, g, level, i : i + size, :] for g in range(4)]
                im = [columns[c, g, level, rows + i : rows + i + size, :] for g in range(4)]
                re_even, re_odd = re[0] + re[2], re[0] - re[2]
                im_even, im_odd = im[0] + im[2], im[0] - im[2]
                re_sum, re_gap = re[1] + re[3], re[1] - re[3]
                im_sum, im_gap = im[1] + im[3], im[1] - im[3]
                legs = (
                    (re_even + re_sum, im_even + im_sum),
                    (re_odd + im_gap, im_odd - re_gap),
                    (re_even - re_sum, im_even - im_sum),
                    (re_odd - im_gap, im_odd + re_gap),
                )
                for r, (a, b) in enumerate(legs):
                    cos = twiddle[r : r + 1, :]
                    sin = twiddle[gy + r : gy + r + 1, :]
                    for part, value in enumerate((a * cos + b * sin, b * cos - a * sin)):
                        at = part * gy * span + r * span + level * rows + i
                        high, low = split_halves(value)
                        z_high[at : at + size, :] = high
                        z_low[at : at + size, :] = low

        def one(step, carry):
            o = turn(step)
            to = partner(my, o)
            table = y_high[to]
            terms = mxu(z_high[...], table) + mxu(z_low[...], table) + mxu(z_high[...], y_low[to])
            half = gy * span
            wide = y_local // gy
            re = terms[:half, :wide] + terms[half:, wide:]
            im = terms[half:, :wide] - terms[:half, wide:]
            whole = jnp.concatenate(
                [
                    jnp.concatenate([piece[r * span : (r + 1) * span] for r in range(gy)], axis=1)
                    for piece in (re, im)
                ],
                axis=0,
            )
            high, low = split_halves(whole)
            ordered = mxu(high, order[...]) + mxu(low, order[...])
            spectra[c, o] = ordered.reshape(2, levels, rows, y_local)
            remote, local = copy_d(c, o)
            pl.when(o != 0)(lambda: remote().start())
            pl.when(o == 0)(lambda: local().start())
            return carry

        lax.fori_loop(0, gy, one, 0)

    barrier = pltpu.get_barrier_semaphore()
    lone = lone_at(me, my)

    def greet(semaphore, axis, target):
        pl.semaphore_signal(
            semaphore, inc=1, device_id={axis: target}, device_id_type=MESH_IDS
        )

    greet(barrier, "gy", partner(my, gy - 1))
    for o in range(1, gy - 1):
        to = partner(my, o)
        pl.when(lone_at(me, to) == 0)(functools.partial(greet, barrier, "gy", to))
    for o in range(1, gx):
        to = partner(me, o)
        pl.when(lone_at(to, my) == 0)(functools.partial(greet, barrier, "gx", to))
    pl.semaphore_wait(barrier, 1 + (1 - lone) * (gx + gy - 3))
    start_all(copy_r, 0, (gy - 1,))
    stages = [
        pltpu.make_async_copy(
            fields.at[first * levels + partner(my, o)], staged.at[o - 1], stage_sem.at[o - 1]
        )
        for o in (1, 2)
    ]
    for stage in stages:
        stage.start()

    def release():
        for o in range(1, gy - 1):
            to = partner(my, o)
            pl.when(lone_at(me, to) * (1 - inner_at(my)) == 1)(
                functools.partial(greet, go, "gy", to)
            )
        for o in range(1, gx):
            to = partner(me, o)
            pl.when(lone_at(to, my) == 1)(functools.partial(greet, go, "gx", to))

    pl.when(lone == 0)(release)
    pl.when(lone == 1)(lambda: pl.semaphore_wait(go, gx // 2 + gy // 2))
    for stage in stages:
        stage.wait()
    start_all(copy_r, 0, y_order[1:])
    start_all(copy_a, 0, x_order)
    tables = [
        pltpu.make_async_copy(src, dst, table_sem.at[i])
        for i, (src, dst) in enumerate(
            (
                (order_rows_in, order_rows),
                (twiddle_in, twiddle),
                (y_high_in, y_high),
                (y_low_in, y_low),
                (order_in, order),
            )
        )
    ]
    for table in tables:
        table.start()
    tables[0].wait()
    for i in range(order_rows.shape[0]):
        row = jnp.broadcast_to(order_rows[i : i + 1, :], (LANES, LANES))
        order_column[i * LANES : (i + 1) * LANES, :] = row.T
    lax.fori_loop(0, x_high.shape[0] // (2 * rows), make_table, 0)
    for table in tables[1:]:
        table.wait()

    def forward(c):
        arrive(first_b, c, x_order)
        start_all(copy_c, c, (3, 2))
        arrive(late_b, c, x_order)
        start_all(copy_c, c, (1, 0))

    def lines_stage(c):
        arrive(copy_a, c, x_order)
        x_stage(c)

    def columns_stage(c):
        arrive(copy_c, c, y_order)
        y_stage(c)

    lines_stage(0)
    start_all(copy_a, 1, x_order)
    forward(0)
    lines_stage(1)
    arrive(copy_r, 0, y_order)
    start_all(copy_a, 2, x_order)
    start_all(copy_a, 3, x_order)
    forward(1)
    columns_stage(0)
    lines_stage(2)
    lines_stage(3)
    columns_stage(1)
    for c in (2, 3):
        arrive(first_b, c, x_order)
        arrive(late_b, c, x_order)
    y_stage(2)
    y_stage(3)

    def sent(copy, c, offsets):
        for o in offsets:
            if o:
                copy(c, o)[0]().wait_send()

    for c in range(chunks):
        arrive(copy_d, c, y_order)
    sent(copy_r, 0, y_order)
    for c in range(chunks):
        for copy in (copy_a, first_b, late_b):
            sent(copy, c, x_order)
        if c < first:
            sent(copy_c, c, y_order)
        sent(copy_d, c, y_order)


def keep_kernel(scale, spectra, kept_mask, out, kept, sems):
    copies = []
    for piece in range(spectra.shape[0]):
        kept[piece] = spectra[piece] * (kept_mask[...].astype(jnp.float32) * scale)
        copies.append(pltpu.make_async_copy(kept.at[piece], out.at[piece], sems.at[piece]))
        copies[-1].start()
    for copy in copies:
        copy.wait()


def stay(value):
    return pltpu.with_memory_space_constraint(value, pltpu.HBM)


def kernel_shards(gx, gy, fields, wave_order, kept_mask):
    stack, x_local, y_local = fields.shape
    nx, ny = x_local * gx, y_local * gy
    levels = gx * LANES // y_local
    chunks = stack // levels
    rows = wave_order.shape[0] // (gx * gy)
    all_rows = 2 * wave_order.shape[0]
    twiddle, y_high, y_low, order = y_tables(y_local, gy)
    order_rows = wave_order.reshape(-1, LANES)
    vmem = pl.BlockSpec(memory_space=pltpu.VMEM)
    anywhere = pl.BlockSpec(memory_space=pl.ANY)
    hbm = pl.BlockSpec(memory_space=pl.ANY)
    z_rows = 2 * gy * levels * rows
    spectra = pl.pallas_call(
        functools.partial(exchange_kernel, gx, gy, levels, chunks),
        out_shape=pltpu.VMEM((2, stack, gy, rows, y_local), jnp.float32),
        in_specs=[hbm] * 6,
        out_specs=anywhere,
        scratch_shapes=[
            pltpu.VMEM((2, x_local, y_local), jnp.float32),
            pltpu.VMEM(order_rows.shape, jnp.int32),
            pltpu.VMEM(twiddle.shape, jnp.float32),
            pltpu.VMEM((wave_order.shape[0], LANES), jnp.int32),
            pltpu.VMEM((all_rows, nx), jnp.bfloat16),
            pltpu.VMEM((all_rows, nx), jnp.bfloat16),
            pltpu.VMEM((chunks, nx, LANES), jnp.float32),
            pltpu.VMEM((nx, 2 * LANES), jnp.bfloat16),
            pltpu.VMEM((chunks, gx, gy, 2 * rows, LANES), jnp.float32),
            pltpu.VMEM((chunks, gy, levels, 2 * rows, y_local), jnp.float32),
            pltpu.VMEM((chunks, gy, levels, 2 * rows, y_local), jnp.float32),
            pltpu.VMEM((z_rows, y_local), jnp.bfloat16),
            pltpu.VMEM((z_rows, y_local), jnp.bfloat16),
            pltpu.VMEM((chunks, gy, 2, levels, rows, y_local), jnp.float32),
            pltpu.VMEM(y_high.shape, jnp.bfloat16),
            pltpu.VMEM(y_low.shape, jnp.bfloat16),
            pltpu.VMEM(order.shape, jnp.bfloat16),
            pltpu.VMEM((gy, x_local, y_local), jnp.float32),
        ]
        + [pltpu.SemaphoreType.DMA((1, gy))] * 2
        + [pltpu.SemaphoreType.DMA((chunks, gx))] * 2
        + [pltpu.SemaphoreType.DMA((2, chunks, gx))] * 2
        + [pltpu.SemaphoreType.DMA((chunks, gy))] * 4
        + [pltpu.SemaphoreType.DMA((5,)), pltpu.SemaphoreType.DMA((2,)), pltpu.SemaphoreType.REGULAR],
        compiler_params=pltpu.CompilerParams(
            collective_id=0, has_side_effects=True, vmem_limit_bytes=58 * 1024 * 1024
        ),
        name="exchange",
    )(*map(stay, (fields, order_rows, twiddle, y_high, y_low, order)))
    pieces = 2 * stack
    kept = pl.pallas_call(
        functools.partial(keep_kernel, 1.0 / math.sqrt(nx * ny)),
        out_shape=jax.ShapeDtypeStruct((pieces, gy * rows, y_local), jnp.float32),
        in_specs=[vmem, vmem],
        out_specs=anywhere,
        scratch_shapes=[
            pltpu.VMEM((pieces, gy * rows, y_local), jnp.float32),
            pltpu.SemaphoreType.DMA((pieces,)),
        ],
        compiler_params=pltpu.CompilerParams(vmem_limit_bytes=6 * 1024 * 1024),
        name="keep",
    )(spectra.reshape(pieces, gy * rows, y_local), kept_mask)
    return kept.reshape(2, stack, gy * rows, y_local)


def kernel_fits(gx, gy):
    y_local, x_local = NY // gy, NX // gx
    if gx != 8 or gy != 4 or NX & (NX - 1) or y_local % (4 * LANES) or x_local % LANES or gx * LANES % y_local:
        return False
    levels = gx * LANES // y_local
    return STACK == 4 * levels == 2 * gy and KX % (gx * gy * 16) == 0


def solution(mesh):
    gx, gy = mesh.shape["gx"], mesh.shape["gy"]
    body = functools.partial(kernel_shards, gx, gy) if kernel_fits(gx, gy) else shards
    return jax.shard_map(
        body,
        mesh=mesh,
        in_specs=(P(None, "gx", "gy"), P(), P("gx", "gy")),
        out_specs=P(None, None, "gx", "gy"),
        check_vma=False,
    )
```
